16 devices in a mesh: data: 4 (over z, y), seq: 4 (over x, core).
Axes of the slice: x: 2, y: 2, z: 2, core: 2. Of those that a mesh axis runs over, the one named last changes fastest.
Arguments:
- x: bfloat16 [8192, 4096], P(('data', 'seq')), parts along dimension 0
- g1: float32 [4096], replicated
- b1: float32 [4096], replicated
- g2: float32 [4096], replicated
- b2: float32 [4096], replicated
- wqkv: bfloat16 [4096, 12288], replicated
- wo: bfloat16 [32, 128, 4096], replicated
- w1: bfloat16 [4096, 16384], replicated
- w2: bfloat16 [16384, 4096], replicated
Outputs:
- output: bfloat16 [8192, 4096], P(('data', 'seq')), parts along dimension 0
There are 4 independent parts. The reference program is written for one: setup_inputs(seed, part) draws one part's arguments, and reference() takes and returns one part's arrays. A program takes and returns all parts, laid end to end along the dimension named above; an argument that names none is the same for every part.
All inputs are finite; a program needn't handle non-finite values.
Results may differ from the reference program's by a relative error of at most 0.00239018.
Values are sent between devices in bfloat16 or wider.
A program may use at most 1.75 GiB of HBM per device.

```python
import jax
import jax.numpy as jnp
from jax import lax

S = 2048
D = 4096
H = 32
DH = 128
F = 16384
QB = 128

EPS = 1e-5
SCALE = DH ** -0.5
NEG = -1e30


def setup_inputs(seed: int = 0, part: int = 0) -> dict:
    key = jax.random.PRNGKey(seed)
    k_shared, k_part = jax.random.split(key)
    kp = jax.random.fold_in(k_part, part)
    kx, ku, kf, kph = jax.random.split(kp, 4)
    ks = jax.random.split(k_shared, 8)
    nf = 4
    t = jnp.arange(S, dtype=jnp.float32) / S
    freq = jax.random.uniform(kf, (nf,), jnp.float32, 0.25, 2.0)
    phase = jax.random.uniform(kph, (nf,), jnp.float32, 0.0, 6.2831853)
    waves = jnp.sin(6.2831853 * freq[None, :] * t[:, None] + phase[None, :])
    u = jax.random.normal(ku, (nf, D), jnp.float32)
    smooth = jnp.dot(waves, u) * (2.0 / nf) ** 0.5
    x = 0.6 * jax.random.normal(kx, (S, D), jnp.float32) + smooth

    def w(k, shape, fan_in):
        return (jax.random.normal(k, shape, jnp.float32) * fan_in ** -0.5).astype(jnp.bfloat16)

    return {
        "x": x.astype(jnp.bfloat16),
        "g1": 1.0 + 0.2 * jax.random.normal(ks[0], (D,), jnp.float32),
        "b1": 0.2 * jax.random.normal(ks[1], (D,), jnp.float32),
        "g2": 1.0 + 0.2 * jax.random.normal(ks[2], (D,), jnp.float32),
        "b2": 0.2 * jax.random.normal(ks[3], (D,), jnp.float32),
        "wqkv": w(ks[4], (D, 3 * H * DH), D),
        "wo": w(ks[5], (H, DH, D), H * DH),
        "w1": w(ks[6], (D, F), D),
        "w2": w(ks[7], (F, D), F),
    }


def _layer_norm(x, g, b):
    xf = x.astype(jnp.float32)
    mu = jnp.mean(xf, axis=-1, keepdims=True)
    var = jnp.mean(jnp.square(xf - mu), axis=-1, keepdims=True)
    return ((xf - mu) * lax.rsqrt(var + EPS) * g + b).astype(jnp.bfloat16)


def _rope(t, pos):
    half = DH // 2
    inv = 10000.0 ** (-2.0 * jnp.arange(half, dtype=jnp.float32) / DH)
    ang = pos.astype(jnp.float32)[:, None] * inv[None, :]
    cos = jnp.cos(ang)[:, None, :]
    sin = jnp.sin(ang)[:, None, :]
    tf = t.astype(jnp.float32)
    a, b = tf[..., :half], tf[..., half:]
    return jnp.concatenate([a * cos - b * sin, b * cos + a * sin], axis=-1).astype(jnp.bfloat16)


def _head_attention(qh, kh, vh):
    rows = jnp.arange(S).reshape(S // QB, QB)
    cols = jnp.arange(S)

    def block(args):
        qb, rb = args
        s = jnp.dot(qb, kh.T, preferred_element_type=jnp.float32) * SCALE
        s = jnp.where(cols[None, :] <= rb[:, None], s, NEG)
        p = jax.nn.softmax(s, axis=-1).astype(jnp.bfloat16)
        return jnp.dot(p, vh, preferred_element_type=jnp.float32).astype(jnp.bfloat16)

    return lax.map(block, (qh.reshape(S // QB, QB, DH), rows)).reshape(S, DH)


def reference(x, g1, b1, g2, b2, wqkv, wo, w1, w2):
    pos = jnp.arange(S)
    a = _layer_norm(x, g1, b1)
    qkv = jnp.dot(a, wqkv, preferred_element_type=jnp.float32).astype(jnp.bfloat16).reshape(S, 3, H, DH)
    q = _rope(qkv[:, 0], pos)
    k = _rope(qkv[:, 1], pos)
    v = qkv[:, 2]
    o = lax.map(lambda t: _head_attention(t[0], t[1], t[2]),
                (q.transpose(1, 0, 2), k.transpose(1, 0, 2), v.transpose(1, 0, 2)))
    o = o.transpose(1, 0, 2).reshape(S, H * DH)
    attn = jnp.dot(o, wo.reshape(H * DH, D), preferred_element_type=jnp.float32)
    m = _layer_norm(x, g2, b2)
    h = jax.nn.gelu(jnp.dot(m, w1, preferred_element_type=jnp.float32), approximate=False).astype(jnp.bfloat16)
    mlp = jnp.dot(h, w2, preferred_element_type=jnp.float32)
    return (x.astype(jnp.float32) + attn + mlp).astype(jnp.bfloat16)
```

```python
import jax
import jax.numpy as jnp
from jax import lax
from jax.experimental import pallas as pl
from jax.experimental.pallas import tpu as pltpu
from jax.sharding import PartitionSpec as P

EPS = 1e-5
NEG = -1e30
F32 = jnp.float32
BF16 = jnp.bfloat16
VMEM = 60 * 1024 * 1024


def _params(n):
    return pltpu.CompilerParams(dimension_semantics=("arbitrary",) * n, vmem_limit_bytes=VMEM)


def _cost(flops, nbytes):
    return pl.CostEstimate(flops=int(flops), bytes_accessed=int(nbytes), transcendentals=0)


def _dot(a, b):
    return jnp.dot(a, b, preferred_element_type=F32)


def _norms(x, g1, b1, g2, b2):
    r, d = x.shape
    tr = 128

    def body(x_ref, g1_ref, b1_ref, g2_ref, b2_ref, a_ref, m_ref):
        xf = x_ref[...].astype(F32)
        mu = jnp.mean(xf, axis=-1, keepdims=True)
        xc = xf - mu
        var = jnp.mean(xc * xc, axis=-1, keepdims=True)
        xn = xc * lax.rsqrt(var + EPS)
        a_ref[...] = (xn * g1_ref[...] + b1_ref[...]).astype(BF16)
        m_ref[...] = (xn * g2_ref[...] + b2_ref[...]).astype(BF16)

    row = pl.BlockSpec((tr, d), lambda i: (i, 0))
    vec = pl.BlockSpec((1, d), lambda i: (0, 0))
    out = jax.ShapeDtypeStruct((r, d), BF16)
    return pl.pallas_call(
        body, grid=(r // tr,), in_specs=[row, vec, vec, vec, vec], out_specs=[row, row],
        out_shape=[out, out], compiler_params=_params(1), name="norms",
        cost_estimate=_cost(20 * r * d, 6 * r * d),
    )(x, g1[None], b1[None], g2[None], b2[None])


def _rope_tables(s, dh):
    half = dh // 2
    e = lax.broadcasted_iota(jnp.int32, (1, dh), 1)
    inv = 10000.0 ** (-2.0 * (e % half).astype(F32) / dh)
    ang = jnp.arange(s).astype(F32)[:, None] * inv
    sin = jnp.sin(ang)
    return jnp.cos(ang), jnp.where(e < half, -sin, sin)


def _qkv(me, ks, blocks, cos, sin, wqkv, buf):
    r, d = blocks[0].shape
    nh3 = wqkv.shape[1]
    dh = cos.shape[1]
    w3 = nh3 // 3
    hw = w3 // 4
    nt = 512
    nb = hw // nt
    na = len(blocks)

    def body(me_ref, *refs):
        a_refs, (cos_ref, sin_ref, w_ref), out_ref = refs[:na], refs[na:na + 3], refs[-1]
        isv = pl.program_id(0) == 2
        for k, a_ref in zip(ks, a_refs):
            blk = ((me_ref[0] ^ k) % 2) if na == 2 else 0
            rows = pl.ds(pl.multiple_of(blk * r, r), r)
            cs, sn = cos_ref[rows, :], sin_ref[rows, :]
            for c in range(nt // 256):
                t = _dot(a_ref[...], w_ref[:, c * 256:(c + 1) * 256]).astype(BF16).astype(F32)
                for h in range(256 // dh):
                    u = t[:, h * dh:(h + 1) * dh]
                    v = u * cs + pltpu.roll(u, dh // 2, 1) * sn
                    lo = c * 256 + h * dh
                    out_ref[rows, lo:lo + dh] = jnp.where(isv, u, v).astype(BF16)

    def place(m):
        return (m[0] ^ ks[0]) // na

    whole = pl.BlockSpec((r, d), lambda t, j, m: (0, 0))
    tab = pl.BlockSpec((na * r, dh), lambda t, j, m: (place(m), 0))
    in_specs = [whole] * na + [
        tab, tab, pl.BlockSpec((d, nt), lambda t, j, m: (0, (t * 4 + m[0]) * nb + j))]
    args = [me, *blocks, cos, sin, wqkv]
    alias = {}
    if buf is not None:
        in_specs.append(pl.BlockSpec(memory_space=pl.ANY))
        args.append(buf)
        alias = {len(args) - 1: 0}
    return pl.pallas_call(
        body,
        grid_spec=pltpu.PrefetchScalarGridSpec(
            num_scalar_prefetch=1, grid=(3, nb), in_specs=in_specs,
            out_specs=pl.BlockSpec((na * r, nt), lambda t, j, m: (place(m), t * nb + j))),
        out_shape=jax.ShapeDtypeStruct((4 * r, 3 * hw), BF16),
        input_output_aliases=alias, compiler_params=_params(2), name="qkv" + "".join(map(str, ks)),
        cost_estimate=_cost(2 * na * r * d * 3 * hw, 2 * d * 3 * hw + 2 * na * r * d),
    )(*args)


def _attention(me, qkv, dh):
    s, w = qkv.shape
    hw = w // 3
    nh = hw // dh
    qb = 256
    r = s // 4
    c2 = dh ** -0.5 * 1.4426950408889634

    def body(me_ref, q_ref, k_ref, v_ref, o0, o1, o2, o3, o_scr):
        row = lax.broadcasted_iota(jnp.int32, (qb, qb), 0)
        col = lax.broadcasted_iota(jnp.int32, (qb, qb), 1)
        keep = col <= row
        for b in range(s // qb):
            n = b * qb
            q = q_ref[n:n + qb, :]
            dn = (((1,), (1,)), ((), ()))
            sd = lax.dot_general(q, k_ref[n:n + qb, :], dn, preferred_element_type=F32)
            sd = jnp.where(keep, sd, NEG)
            m = jnp.max(sd, axis=-1, keepdims=True)
            if n:
                sp = lax.dot_general(q, k_ref[:n, :], dn, preferred_element_type=F32)
                m = jnp.maximum(m, jnp.max(sp, axis=-1, keepdims=True))
            p = jnp.exp2((sd - m) * c2)
            l = jnp.sum(p, axis=-1, keepdims=True)
            o = _dot(p.astype(BF16), v_ref[n:n + qb, :])
            if n:
                p = jnp.exp2((sp - m) * c2)
                l = l + jnp.sum(p, axis=-1, keepdims=True)
                o = o + _dot(p.astype(BF16), v_ref[:n, :])
            o_scr[n:n + qb, :] = (o / l).astype(BF16)
        for k, o_ref in enumerate((o0, o1, o2, o3)):
            o_ref[...] = o_scr[pl.ds(pl.multiple_of((me_ref[0] ^ k) * r, r), r), :]

    def col(base):
        return pl.BlockSpec((s, dh), lambda h, m: (0, base + h))

    out = jax.ShapeDtypeStruct((r, hw), BF16)
    ospec = pl.BlockSpec((r, dh), lambda h, m: (0, h))
    return pl.pallas_call(
        body,
        grid_spec=pltpu.PrefetchScalarGridSpec(
            num_scalar_prefetch=1, grid=(nh,), in_specs=[col(0), col(nh), col(2 * nh)],
            out_specs=[ospec] * 4, scratch_shapes=[pltpu.VMEM((s, dh), BF16)]),
        out_shape=[out] * 4, compiler_params=_params(1), name="attention",
        cost_estimate=_cost(4 * s * s * dh * nh, 8 * s * hw),
    )(me, qkv, qkv, qkv)


def _mlp1(m, w1):
    r, d = m.shape
    f = w1.shape[1]
    nt = 512

    def body(m_ref, w_ref, h_ref):
        for c in range(nt // 256):
            cols = slice(c * 256, (c + 1) * 256)
            t = _dot(m_ref[...], w_ref[:, cols])
            h_ref[:, cols] = (0.5 * t * (1.0 + lax.erf(t * (0.5 ** 0.5)))).astype(BF16)

    return pl.pallas_call(
        body, grid=(f // nt,),
        in_specs=[pl.BlockSpec((r, d), lambda j: (0, 0)), pl.BlockSpec((d, nt), lambda j: (0, j))],
        out_specs=pl.BlockSpec((r, nt), lambda j: (0, j)),
        out_shape=jax.ShapeDtypeStruct((r, f), BF16), compiler_params=_params(1), name="mlp1",
        cost_estimate=_cost(2 * r * d * f, 2 * d * f + 2 * r * f),
    )(m, w1)


def _mlp2(h, w2):
    r, f = h.shape
    d = w2.shape[1]
    nt = 256

    def body(h_ref, w_ref, o_ref):
        o_ref[...] = _dot(h_ref[...], w_ref[...])

    return pl.pallas_call(
        body, grid=(d // nt,),
        in_specs=[pl.BlockSpec((r, f), lambda j: (0, 0)), pl.BlockSpec((f, nt), lambda j: (0, j))],
        out_specs=pl.BlockSpec((r, nt), lambda j: (0, j)),
        out_shape=jax.ShapeDtypeStruct((r, d), F32), compiler_params=_params(1), name="mlp2",
        cost_estimate=_cost(2 * r * d * f, 2 * d * f + 2 * r * f),
    )(h, w2)


def _final(me, x, part, os, wo):
    r, d = x.shape
    hw = os[0].shape[1]
    nt = 512

    def body(me_ref, x_ref, p_ref, o0, o1, o2, o3, w_ref, y_ref):
        acc = None
        for k, o_ref in enumerate((o0, o1, o2, o3)):
            rows = pl.ds(pl.multiple_of((me_ref[0] ^ k) * hw, hw), hw)
            t = _dot(o_ref[...], w_ref[rows, :])
            acc = t if acc is None else acc + t
        y_ref[...] = (x_ref[...].astype(F32) + acc + p_ref[...]).astype(BF16)

    tile = pl.BlockSpec((r, nt), lambda j, m: (0, j))
    whole = pl.BlockSpec((r, hw), lambda j, m: (0, 0))
    return pl.pallas_call(
        body,
        grid_spec=pltpu.PrefetchScalarGridSpec(
            num_scalar_prefetch=1, grid=(d // nt,),
            in_specs=[tile, tile, whole, whole, whole, whole,
                      pl.BlockSpec((4 * hw, nt), lambda j, m: (0, j))],
            out_specs=tile),
        out_shape=jax.ShapeDtypeStruct((r, d), BF16), compiler_params=_params(1), name="final",
        cost_estimate=_cost(2 * r * d * 4 * hw, 2 * d * 4 * hw + 8 * r * d),
    )(me, x, part, *os, wo)


def solution(mesh):
    nseq = mesh.shape["seq"]

    def swap(t, k):
        return lax.ppermute(t, "seq", [(i, i ^ k) for i in range(nseq)])

    def local(x, g1, b1, g2, b2, wqkv, wo, w1, w2):
        nh, dh, d = wo.shape
        r = x.shape[0]
        me = lax.axis_index("seq").astype(jnp.int32)[None]
        a, m = _norms(x, g1, b1, g2, b2)
        a1 = swap(a, 1)
        a2 = swap(a, 2)
        cos, sin = _rope_tables(nseq * r, dh)
        h = _mlp1(m, w1)
        qkv = _qkv(me, (0, 1), (a, a1), cos, sin, wqkv, None)
        a2, qkv, h = lax.optimization_barrier((a2, qkv, h))
        a3 = swap(a2, 1)
        qkv = _qkv(me, (2,), (a2,), cos, sin, wqkv, qkv)
        qkv = _qkv(me, (3,), (a3,), cos, sin, wqkv, qkv)
        os = _attention(me, qkv, dh)
        os = [os[0]] + [swap(os[k], k) for k in range(1, nseq)]
        part = _mlp2(h, w2)
        return _final(me, x, part, os, wo.reshape(nh * dh, d))

    rows = P(("data", "seq"), None)
    rep = P()
    return jax.shard_map(local, mesh=mesh,
                         in_specs=(rows, rep, rep, rep, rep, rep, rep, rep, rep),
                         out_specs=rows, check_vma=False)
```

```python
import jax
import jax.numpy as jnp
from jax import lax
from jax.experimental import pallas as pl
from jax.experimental.pallas import tpu as pltpu
from jax.sharding import PartitionSpec as P

EPS = 1e-5
NEG = -1e30
F32 = jnp.float32
BF16 = jnp.bfloat16
VMEM = 60 * 1024 * 1024


def _params(n):
    return pltpu.CompilerParams(dimension_semantics=("arbitrary",) * n, vmem_limit_bytes=VMEM)


def _cost(flops, nbytes):
    return pl.CostEstimate(flops=int(flops), bytes_accessed=int(nbytes), transcendentals=0)


def _dot(a, b):
    return jnp.dot(a, b, preferred_element_type=F32)


MESH = pl.DeviceIdType.MESH
LO = 64


def _rope_tables(s, dh):
    half = dh // 2
    e = lax.broadcasted_iota(jnp.int32, (1, dh), 1)
    inv = 10000.0 ** (-2.0 * (e % half).astype(F32) / dh)
    lo = jnp.arange(LO).astype(F32)[:, None] * inv
    hi = (LO * jnp.arange(s // LO)).astype(F32)[:, None] * inv
    return jnp.cos(lo), jnp.sin(lo), jnp.cos(hi), jnp.sin(hi)


def _front(x, g1, b1, g2, b2, tabs, wqkv, w1):
    r, d = x.shape
    f = w1.shape[1]
    w3 = wqkv.shape[1] // 3
    hw = w3 // 4
    dh = tabs[0].shape[1]
    nt = 512
    mt = 2 * nt
    cw = 256
    t1 = f // mt
    nb = hw // nt
    t2 = 3 * nb
    ntile1 = f // nt
    ntiles = ntile1 + 2 * t2
    ring = 5
    xc = 128
    steps = t1 + 2 * t2

    def body(x_ref, g1_ref, b1_ref, g2_ref, b2_ref, cl, sl, ch, sh, wqkv_ref, w1_ref,
             h_ref, qkv_ref, rows, m_scr, w_scr, t_scr, cos_s, sin_s,
             xsem, wsem, send, recv):
        s = pl.program_id(0)
        me = lax.axis_index("seq")
        core = me % 2
        near = me + 1 - 2 * core
        far = (me + 2) % 4

        def member(k):
            return [me, near, far, 3 - me][k]

        def load(i):
            slot = i % ring

            @pl.when(i < ntile1)
            def _():
                c = pl.multiple_of(i * nt, nt)
                pltpu.make_async_copy(w1_ref.at[:, pl.ds(c, nt)], w_scr.at[slot], wsem.at[slot]).start()

            @pl.when((i >= ntile1) & (i < ntiles))
            def _():
                v = (i - ntile1) % t2
                c = pl.multiple_of((v // nb) * w3 + me * hw + (v % nb) * nt, nt)
                pltpu.make_async_copy(wqkv_ref.at[:, pl.ds(c, nt)], w_scr.at[slot], wsem.at[slot]).start()

        def ready(i):
            slot = i % ring
            pltpu.make_async_copy(w1_ref.at[:, pl.ds(0, nt)], w_scr.at[slot], wsem.at[slot]).wait()
            return slot

        def remote(src, dst, sem, dev):
            return pltpu.make_async_remote_copy(
                src_ref=rows.at[src], dst_ref=rows.at[dst], send_sem=send.at[sem],
                recv_sem=recv.at[sem], device_id={"seq": dev}, device_id_type=MESH)

        def to_near():
            return remote(0, 1, 0, near)

        def to_far():
            return remote(0, 2, 1, far)

        def onward():
            return remote(2, 3, 2, near)

        @pl.when(s == 0)
        def _():
            def chunk(c):
                rs = pl.ds(c * xc, xc)
                return pltpu.make_async_copy(x_ref.at[rs], rows.at[0, rs], xsem.at[c])

            for c in range(r // xc):
                chunk(c).start()
            for i in range(ring):
                load(i)
            bar = pltpu.get_barrier_semaphore()
            for dev in (near, far):
                pl.semaphore_signal(bar, inc=1, device_id={"seq": dev}, device_id_type=MESH)
            for c in range(r // xc):
                chunk(c).wait()

                def norm(q, _):
                    rs = pl.ds(pl.multiple_of(c * xc + q * 16, 16), 16)
                    xf = rows[0, rs, :].astype(F32)
                    mu = jnp.mean(xf, axis=-1, keepdims=True)
                    xm = xf - mu
                    var = jnp.mean(xm * xm, axis=-1, keepdims=True)
                    xn = xm * lax.rsqrt(var + EPS)
                    rows[0, rs, :] = (xn * g1_ref[...] + b1_ref[...]).astype(BF16)
                    m_scr[rs, :] = (xn * g2_ref[...] + b2_ref[...]).astype(BF16)
                    return 0

                lax.fori_loop(0, xc // 16, norm, 0, unroll=2)
            pl.semaphore_wait(bar, 2)
            to_far().start()
            to_near().start()
            neg = lax.broadcasted_iota(jnp.int32, (LO, dh), 1) < dh // 2
            for k in range(4):
                n = r // LO
                base = pl.ds(pl.multiple_of(member(k) * n, n), n)
                hc, hs = ch[base, :], sh[base, :]
                for i in range(n):
                    a, b = hc[i:i + 1], hs[i:i + 1]
                    sn = b * cl[...] + a * sl[...]
                    cos_s[k, i * LO:(i + 1) * LO, :] = a * cl[...] - b * sl[...]
                    sin_s[k, i * LO:(i + 1) * LO, :] = jnp.where(neg, -sn, sn)

        def gelu(cols):
            t = t_scr[:, cols]
            h_ref[:, cols] = (0.5 * t * (1.0 + lax.erf(t * (0.5 ** 0.5)))).astype(BF16)

        def mlp(first):
            slots = [ready(2 * s + half) for half in range(mt // nt)]
            for half, slot in enumerate(slots):
                for c in range(nt // cw):
                    cols = slice(half * nt + c * cw, half * nt + (c + 1) * cw)
                    if not first:
                        gelu(cols)
                    t_scr[:, cols] = _dot(m_scr[...], w_scr[slot, :, c * cw:(c + 1) * cw])
            load(2 * s + ring)
            load(2 * s + ring + 1)

        pl.when(s == 0)(lambda: mlp(True))
        pl.when((s > 0) & (s < t1))(lambda: mlp(False))

        def qkv(first):
            u = s - t1
            i = ntile1 + u
            slot = ready(i)
            isv = (u % t2) // nb == 2
            base = 2 * (u // t2)
            for k in range(2):
                out = pl.ds(pl.multiple_of((core if k == 0 else 1 - core) * r, r), r)
                a = rows.at[base + k]
                for c in range(nt // cw):
                    if first:
                        gelu(slice((2 * k + c) * cw, (2 * k + c + 1) * cw))
                    t = _dot(a[...], w_scr[slot, :, c * cw:(c + 1) * cw]).astype(BF16).astype(F32)
                    for hd in range(cw // dh):
                        p = t[:, hd * dh:(hd + 1) * dh]
                        v = p * cos_s[base + k] + pltpu.roll(p, dh // 2, 1) * sin_s[base + k]
                        lo = c * cw + hd * dh
                        qkv_ref[out, lo:lo + dh] = jnp.where(isv, p, v).astype(BF16)
            load(i + ring)

        @pl.when(s == t1)
        def _():
            to_near().wait_recv()
            qkv(True)

        @pl.when(s == t1 + t2 // 2)
        def _():
            to_far().wait_recv()
            onward().start()

        @pl.when(s == t1 + t2)
        def _():
            onward().wait_recv()

        pl.when(s > t1)(lambda: qkv(False))

        @pl.when(s == steps - 1)
        def _():
            to_near().wait_send()
            to_far().wait_send()
            onward().wait_send()

    def h_map(s):
        return 0, jnp.clip(s - 1, 0, t1 - 1)

    def qkv_map(s):
        u = jnp.maximum(s - t1, 0)
        chip = lax.axis_index("seq") // 2
        second = u // t2
        return chip + second * (1 - 2 * chip), u % t2

    def full(shape):
        return pl.BlockSpec(shape, lambda s: (0, 0))

    anyspace = pl.BlockSpec(memory_space=pl.ANY)
    return pl.pallas_call(
        body,
        grid=(steps,),
        in_specs=[anyspace] + [full((1, d))] * 4 + [full(t.shape) for t in tabs] + [anyspace] * 2,
        out_specs=[pl.BlockSpec((r, mt), h_map), pl.BlockSpec((2 * r, nt), qkv_map)],
        out_shape=[jax.ShapeDtypeStruct((r, f), BF16), jax.ShapeDtypeStruct((4 * r, 3 * hw), BF16)],
        scratch_shapes=[
            pltpu.VMEM((4, r, d), BF16), pltpu.VMEM((r, d), BF16), pltpu.VMEM((ring, d, nt), BF16),
            pltpu.VMEM((r, mt), F32), pltpu.VMEM((4, r, dh), F32), pltpu.VMEM((4, r, dh), F32),
            pltpu.SemaphoreType.DMA((r // xc,)), pltpu.SemaphoreType.DMA((ring,)),
            pltpu.SemaphoreType.DMA((3,)), pltpu.SemaphoreType.DMA((3,))],
        compiler_params=pltpu.CompilerParams(
            dimension_semantics=("arbitrary",), vmem_limit_bytes=VMEM, collective_id=0,
            has_side_effects=True),
        name="front",
        cost_estimate=_cost(2 * r * d * f + 2 * 4 * r * d * 3 * hw, 2 * d * f + 4 * d * 3 * hw),
    )(x, g1[None], b1[None], g2[None], b2[None], *tabs, wqkv, w1)


def _attention(me, qkv, dh):
    s, w = qkv.shape
    hw = w // 3
    nh = hw // dh
    qb = 256
    r = s // 4
    c2 = dh ** -0.5 * 1.4426950408889634

    def body(me_ref, q_ref, k_ref, v_ref, o0, o1, o2, o3, o_scr):
        row = lax.broadcasted_iota(jnp.int32, (qb, qb), 0)
        col = lax.broadcasted_iota(jnp.int32, (qb, qb), 1)
        keep = col <= row
        for b in range(s // qb):
            n = b * qb
            q = q_ref[n:n + qb, :]
            dn = (((1,), (1,)), ((), ()))
            sd = lax.dot_general(q, k_ref[n:n + qb, :], dn, preferred_element_type=F32)
            sd = jnp.where(keep, sd, NEG)
            m = jnp.max(sd, axis=-1, keepdims=True)
            if n:
                sp = lax.dot_general(q, k_ref[:n, :], dn, preferred_element_type=F32)
                m = jnp.maximum(m, jnp.max(sp, axis=-1, keepdims=True))
            p = jnp.exp2((sd - m) * c2)
            l = jnp.sum(p, axis=-1, keepdims=True)
            o = _dot(p.astype(BF16), v_ref[n:n + qb, :])
            if n:
                p = jnp.exp2((sp - m) * c2)
                l = l + jnp.sum(p, axis=-1, keepdims=True)
                o = o + _dot(p.astype(BF16), v_ref[:n, :])
            o_scr[n:n + qb, :] = (o / l).astype(BF16)
        for k, o_ref in enumerate((o0, o1, o2, o3)):
            o_ref[...] = o_scr[pl.ds(pl.multiple_of((me_ref[0] ^ k) * r, r), r), :]

    def col(base):
        return pl.BlockSpec((s, dh), lambda h, m: (0, base + h))

    out = jax.ShapeDtypeStruct((r, hw), BF16)
    ospec = pl.BlockSpec((r, dh), lambda h, m: (0, h))
    return pl.pallas_call(
        body,
        grid_spec=pltpu.PrefetchScalarGridSpec(
            num_scalar_prefetch=1, grid=(nh,), in_specs=[col(0), col(nh), col(2 * nh)],
            out_specs=[ospec] * 4, scratch_shapes=[pltpu.VMEM((s, dh), BF16)]),
        out_shape=[out] * 4, compiler_params=_params(1), name="attention",
        cost_estimate=_cost(4 * s * s * dh * nh, 8 * s * hw),
    )(me, qkv, qkv, qkv)


def _mlp2(h, w2):
    r, f = h.shape
    d = w2.shape[1]
    nt = 256

    def body(h_ref, w_ref, o_ref):
        o_ref[...] = _dot(h_ref[...], w_ref[...])

    return pl.pallas_call(
        body, grid=(d // nt,),
        in_specs=[pl.BlockSpec((r, f), lambda j: (0, 0)), pl.BlockSpec((f, nt), lambda j: (0, j))],
        out_specs=pl.BlockSpec((r, nt), lambda j: (0, j)),
        out_shape=jax.ShapeDtypeStruct((r, d), F32), compiler_params=_params(1), name="mlp2",
        cost_estimate=_cost(2 * r * d * f, 2 * d * f + 2 * r * f),
    )(h, w2)


def _final(me, x, part, os, wo):
    r, d = x.shape
    hw = os[0].shape[1]
    nt = 512

    def body(me_ref, x_ref, p_ref, o0, o1, o2, o3, w_ref, y_ref):
        acc = None
        for k, o_ref in enumerate((o0, o1, o2, o3)):
            rows = pl.ds(pl.multiple_of((me_ref[0] ^ k) * hw, hw), hw)
            t = _dot(o_ref[...], w_ref[rows, :])
            acc = t if acc is None else acc + t
        y_ref[...] = (x_ref[...].astype(F32) + acc + p_ref[...]).astype(BF16)

    tile = pl.BlockSpec((r, nt), lambda j, m: (0, j))
    whole = pl.BlockSpec((r, hw), lambda j, m: (0, 0))
    return pl.pallas_call(
        body,
        grid_spec=pltpu.PrefetchScalarGridSpec(
            num_scalar_prefetch=1, grid=(d // nt,),
            in_specs=[tile, tile, whole, whole, whole, whole,
                      pl.BlockSpec((4 * hw, nt), lambda j, m: (0, j))],
            out_specs=tile),
        out_shape=jax.ShapeDtypeStruct((r, d), BF16), compiler_params=_params(1), name="final",
        cost_estimate=_cost(2 * r * d * 4 * hw, 2 * d * 4 * hw + 8 * r * d),
    )(me, x, part, *os, wo)


def solution(mesh):
    nseq = mesh.shape["seq"]

    def swap(t, k):
        return lax.ppermute(t, "seq", [(i, i ^ k) for i in range(nseq)])

    def local(x, g1, b1, g2, b2, wqkv, wo, w1, w2):
        nh, dh, d = wo.shape
        r = x.shape[0]
        me = lax.axis_index("seq").astype(jnp.int32)[None]
        h, qkv = _front(x, g1, b1, g2, b2, _rope_tables(nseq * r, dh), wqkv, w1)
        os = _attention(me, qkv, dh)
        os = [os[0]] + [swap(os[k], k) for k in range(1, nseq)]
        part = _mlp2(h, w2)
        return _final(me, x, part, os, wo.reshape(nh * dh, d))

    rows = P(("data", "seq"), None)
    rep = P()
    return jax.shard_map(local, mesh=mesh,
                         in_specs=(rows, rep, rep, rep, rep, rep, rep, rep, rep),
                         out_specs=rows, check_vma=False)
```

```python
import functools

import jax
import jax.numpy as jnp
from jax import lax
from jax.experimental import pallas as pl
from jax.experimental.pallas import tpu as pltpu
from jax.sharding import PartitionSpec as P

EPS = 1e-5
NEG = -1e30
F32 = jnp.float32
BF16 = jnp.bfloat16
VMEM = 60 * 1024 * 1024


def _params(n):
    return pltpu.CompilerParams(dimension_semantics=("arbitrary",) * n, vmem_limit_bytes=VMEM)


def _cost(flops, nbytes):
    return pl.CostEstimate(flops=int(flops), bytes_accessed=int(nbytes), transcendentals=0)


def _dot(a, b):
    return jnp.dot(a, b, preferred_element_type=F32)


MESH = pl.DeviceIdType.MESH
LO = 64


def _rope_tables(s, dh):
    half = dh // 2
    e = lax.broadcasted_iota(jnp.int32, (1, dh), 1)
    inv = 10000.0 ** (-2.0 * (e % half).astype(F32) / dh)
    lo = jnp.arange(LO).astype(F32)[:, None] * inv
    hi = (LO * jnp.arange(s // LO)).astype(F32)[:, None] * inv
    return jnp.cos(lo), jnp.sin(lo), jnp.cos(hi), jnp.sin(hi)


def _front(x, g1, b1, g2, b2, tabs, wqkv, w1):
    r, d = x.shape
    f = w1.shape[1]
    w3 = wqkv.shape[1] // 3
    hw = w3 // 4
    dh = tabs[0].shape[1]
    nt = 512
    mt = 2 * nt
    cw = 256
    t1 = f // mt
    nb = hw // nt
    t2 = 3 * nb
    ntile1 = f // nt
    ntiles = ntile1 + 2 * t2
    ring = 5
    xc = 128
    steps = t1 + 2 * t2 + 1

    def body(x_ref, g1_ref, b1_ref, g2_ref, b2_ref, cl, sl, ch, sh, wqkv_ref, w1_ref,
             h_ref, qkv_ref, x_scr, rows, m_scr, w_scr, t_scr, cos_s, sin_s,
             xsem, wsem, send, recv):
        s = pl.program_id(0)
        me = lax.axis_index("seq")
        core = me % 2
        near = me + 1 - 2 * core
        far = (me + 2) % 4

        def member(k):
            return [me, near, far, 3 - me][k]

        def load(i):
            slot = i % ring

            @pl.when(i < ntile1)
            def _():
                c = pl.multiple_of(i * nt, nt)
                pltpu.make_async_copy(w1_ref.at[:, pl.ds(c, nt)], w_scr.at[slot], wsem.at[slot]).start()

            @pl.when((i >= ntile1) & (i < ntiles))
            def _():
                v = (i - ntile1) % t2
                c = pl.multiple_of((v // nb) * w3 + me * hw + (v % nb) * nt, nt)
                pltpu.make_async_copy(wqkv_ref.at[:, pl.ds(c, nt)], w_scr.at[slot], wsem.at[slot]).start()

        def ready(i):
            slot = i % ring
            pltpu.make_async_copy(w1_ref.at[:, pl.ds(0, nt)], w_scr.at[slot], wsem.at[slot]).wait()
            return slot

        def remote(src, dst, sem, dev):
            return pltpu.make_async_remote_copy(
                src_ref=rows.at[src], dst_ref=rows.at[dst], send_sem=send.at[sem],
                recv_sem=recv.at[sem], device_id={"seq": dev}, device_id_type=MESH)

        def to_near():
            return remote(0, 1, 0, near)

        def to_far():
            return remote(0, 2, 1, far)

        def onward():
            return remote(2, 3, 2, near)

        def norm(c, q, _):
            base = c * xc + q * 32
            groups = [pl.ds(pl.multiple_of(base + 16 * g, 16), 16) for g in range(2)]
            nl = d // 128

            def col(rs, j):
                return x_scr[rs, j * 128:(j + 1) * 128].astype(F32)

            def total(f):
                part = [[None] * 4 for _ in groups]
                for j in range(nl):
                    for g, rs in enumerate(groups):
                        v = f(g, col(rs, j))
                        part[g][j % 4] = v if part[g][j % 4] is None else part[g][j % 4] + v
                return [jnp.sum((p[0] + p[1]) + (p[2] + p[3]), axis=-1, keepdims=True) / d for p in part]

            mu = total(lambda g, v: v)
            var = total(lambda g, v: (v - mu[g]) * (v - mu[g]))
            rs_ = [lax.rsqrt(v + EPS) for v in var]
            for j in range(nl):
                cs = slice(j * 128, (j + 1) * 128)
                for g, rs in enumerate(groups):
                    xn = (col(rs, j) - mu[g]) * rs_[g]
                    rows[0, rs, cs] = (xn * g1_ref[:, cs] + b1_ref[:, cs]).astype(BF16)
                    m_scr[rs, cs] = (xn * g2_ref[:, cs] + b2_ref[:, cs]).astype(BF16)
            return 0

        @pl.when(s == 0)
        def _():
            def chunk(c):
                rs = pl.ds(c * xc, xc)
                return pltpu.make_async_copy(x_ref.at[rs], x_scr.at[rs], xsem.at[c])

            for c in range(r // xc):
                chunk(c).start()
            for i in range(ring):
                load(i)
            bar = pltpu.get_barrier_semaphore()
            for dev in (near, far):
                pl.semaphore_signal(bar, inc=1, device_id={"seq": dev}, device_id_type=MESH)
            for c in range(r // xc):
                chunk(c).wait()

                lax.fori_loop(0, xc // 32, functools.partial(norm, c), 0)
            pl.semaphore_wait(bar, 2)
            to_far().start()
            to_near().start()
            neg = lax.broadcasted_iota(jnp.int32, (LO, dh), 1) < dh // 2
            for k in range(4):
                n = r // LO
                base = pl.ds(pl.multiple_of(member(k) * n, n), n)
                hc, hs = ch[base, :], sh[base, :]
                for i in range(n):
                    a, b = hc[i:i + 1], hs[i:i + 1]
                    sn = b * cl[...] + a * sl[...]
                    cos_s[k, i * LO:(i + 1) * LO, :] = a * cl[...] - b * sl[...]
                    sin_s[k, i * LO:(i + 1) * LO, :] = jnp.where(neg, -sn, sn)

        def gelu(cols):
            t = t_scr[:, cols]
            h_ref[:, cols] = (0.5 * t * (1.0 + lax.erf(t * (0.5 ** 0.5)))).astype(BF16)

        def mlp(first):
            slots = [ready(2 * s + half) for half in range(mt // nt)]
            for half, slot in enumerate(slots):
                for c in range(nt // cw):
                    cols = slice(half * nt + c * cw, half * nt + (c + 1) * cw)
                    if not first:
                        gelu(cols)
                    t_scr[:, cols] = _dot(m_scr[...], w_scr[slot, :, c * cw:(c + 1) * cw])
            load(2 * s + ring)
            load(2 * s + ring + 1)

        pl.when(s == 0)(lambda: mlp(True))
        pl.when((s > 0) & (s < t1))(lambda: mlp(False))

        def rope(j):
            u = s - 1 - t1
            isv = (u % t2) // nb == 2
            base = 2 * (u // t2)
            k, c = j // (nt // cw), j % (nt // cw)
            out = pl.ds(pl.multiple_of((core if k == 0 else 1 - core) * r, r), r)
            t = t_scr[:, j * cw:(j + 1) * cw].astype(BF16).astype(F32)
            for hd in range(cw // dh):
                p = t[:, hd * dh:(hd + 1) * dh]
                v = p * cos_s[base + k] + pltpu.roll(p, dh // 2, 1) * sin_s[base + k]
                lo = c * cw + hd * dh
                qkv_ref[out, lo:lo + dh] = jnp.where(isv, p, v).astype(BF16)

        def qkv(first):
            u = s - t1
            slot = ready(ntile1 + u)
            base = 2 * (u // t2)
            for j in range(mt // cw):
                cols = slice(j * cw, (j + 1) * cw)
                k, c = j // (nt // cw), j % (nt // cw)
                if first:
                    gelu(cols)
                else:
                    rope(j)
                t_scr[:, cols] = _dot(rows[base + k], w_scr[slot, :, c * cw:(c + 1) * cw])
            load(ntile1 + u + ring)

        @pl.when(s == t1)
        def _():
            to_near().wait_recv()
            qkv(True)

        @pl.when(s == t1 + t2 // 2)
        def _():
            to_far().wait_recv()
            onward().start()

        @pl.when(s == t1 + t2)
        def _():
            onward().wait_recv()

        pl.when((s > t1) & (s < steps - 1))(lambda: qkv(False))

        @pl.when(s == steps - 1)
        def _():
            for j in range(mt // cw):
                rope(j)

        @pl.when(s == steps - 1)
        def _():
            to_near().wait_send()
            to_far().wait_send()
            onward().wait_send()

    def h_map(s):
        return 0, jnp.clip(s - 1, 0, t1 - 1)

    def qkv_map(s):
        u = jnp.maximum(s - 1 - t1, 0)
        chip = lax.axis_index("seq") // 2
        second = u // t2
        return chip + second * (1 - 2 * chip), u % t2

    def full(shape):
        return pl.BlockSpec(shape, lambda s: (0, 0))

    anyspace = pl.BlockSpec(memory_space=pl.ANY)
    return pl.pallas_call(
        body,
        grid=(steps,),
        in_specs=[anyspace] + [full((1, d))] * 4 + [full(t.shape) for t in tabs] + [anyspace] * 2,
        out_specs=[pl.BlockSpec((r, mt), h_map), pl.BlockSpec((2 * r, nt), qkv_map)],
        out_shape=[jax.ShapeDtypeStruct((r, f), BF16), jax.ShapeDtypeStruct((4 * r, 3 * hw), BF16)],
        scratch_shapes=[
            pltpu.VMEM((r, d), BF16), pltpu.VMEM((4, r, d), BF16), pltpu.VMEM((r, d), BF16), pltpu.VMEM((ring, d, nt), BF16),
            pltpu.VMEM((r, mt), F32), pltpu.VMEM((4, r, dh), F32), pltpu.VMEM((4, r, dh), F32),
            pltpu.SemaphoreType.DMA((r // xc,)), pltpu.SemaphoreType.DMA((ring,)),
            pltpu.SemaphoreType.DMA((3,)), pltpu.SemaphoreType.DMA((3,))],
        compiler_params=pltpu.CompilerParams(
            dimension_semantics=("arbitrary",), vmem_limit_bytes=VMEM, collective_id=0,
            has_side_effects=True),
        name="front",
        cost_estimate=_cost(2 * r * d * f + 2 * 4 * r * d * 3 * hw, 2 * d * f + 4 * d * 3 * hw),
    )(x, g1[None], b1[None], g2[None], b2[None], *tabs, wqkv, w1)


def _attention(me, qkv, dh):
    s, w = qkv.shape
    hw = w // 3
    nh = hw // dh
    qb = 256
    r = s // 4
    c2 = dh ** -0.5 * 1.4426950408889634
    nblk = s // qb

    def body(me_ref, q_ref, k_ref, v_ref, o0, o1, o2, o3, kt, vx, sc, pb, o_scr):
        @pl.when(pl.program_id(0) == 0)
        def _():
            vx[:, dh:] = jnp.ones((s, dh), BF16)

        for c in range(nblk):
            cols = slice(c * qb, (c + 1) * qb)
            vx[cols, :dh] = v_ref[cols, :]
            kt[:, cols] = k_ref[cols, :].T
        row = lax.broadcasted_iota(jnp.int32, (qb, qb), 0)
        col = lax.broadcasted_iota(jnp.int32, (qb, qb), 1)
        keep = col <= row

        def scores(b):
            q = q_ref[b * qb:(b + 1) * qb, :]
            m = None
            for c in range(b + 1):
                cols = slice(c * qb, (c + 1) * qb)
                t = _dot(q, kt[:, cols])
                if c == b:
                    t = jnp.where(keep, t, NEG)
                sc[b % 2, :, cols] = t
                for g in range(qb // dh):
                    u = t[:, g * dh:(g + 1) * dh]
                    m = u if m is None else jnp.maximum(m, u)
            return jnp.max(m, axis=-1, keepdims=True) * c2

        def finish(b, m):
            n = (b + 1) * qb
            for c in range(b + 1):
                cols = slice(c * qb, (c + 1) * qb)
                pb[b % 2, :, cols] = jnp.exp2(sc[b % 2, :, cols] * c2 - m).astype(BF16)
            o = _dot(pb[b % 2, :, :n], vx[:n, :])
            o_scr[b * qb:n, :] = (o[:, :dh] / o[:, dh:]).astype(BF16)

        m = scores(0)
        for b in range(nblk):
            ahead = scores(b + 1) if b + 1 < nblk else None
            finish(b, m)
            m = ahead
        for k, o_ref in enumerate((o0, o1, o2, o3)):
            o_ref[...] = o_scr[pl.ds(pl.multiple_of((me_ref[0] ^ k) * r, r), r), :]

    def col(base):
        return pl.BlockSpec((s, dh), lambda h, m: (0, base + h))

    out = jax.ShapeDtypeStruct((r, hw), BF16)
    ospec = pl.BlockSpec((r, dh), lambda h, m: (0, h))
    return pl.pallas_call(
        body,
        grid_spec=pltpu.PrefetchScalarGridSpec(
            num_scalar_prefetch=1, grid=(nh,), in_specs=[col(0), col(nh), col(2 * nh)],
            out_specs=[ospec] * 4,
            scratch_shapes=[pltpu.VMEM((dh, s), BF16), pltpu.VMEM((s, 2 * dh), BF16),
                            pltpu.VMEM((2, qb, s), F32), pltpu.VMEM((2, qb, s), BF16),
                            pltpu.VMEM((s, dh), BF16)]),
        out_shape=[out] * 4, compiler_params=_params(1), name="attention",
        cost_estimate=_cost(4 * s * s * dh * nh, 8 * s * hw),
    )(me, qkv, qkv, qkv)


def _mlp2(h, w2):
    r, f = h.shape
    d = w2.shape[1]
    nt = 256

    def body(h_ref, w_ref, o_ref):
        o_ref[...] = _dot(h_ref[...], w_ref[...])

    return pl.pallas_call(
        body, grid=(d // nt,),
        in_specs=[pl.BlockSpec((r, f), lambda j: (0, 0)), pl.BlockSpec((f, nt), lambda j: (0, j))],
        out_specs=pl.BlockSpec((r, nt), lambda j: (0, j)),
        out_shape=jax.ShapeDtypeStruct((r, d), F32), compiler_params=_params(1), name="mlp2",
        cost_estimate=_cost(2 * r * d * f, 2 * d * f + 2 * r * f),
    )(h, w2)


def _final(me, x, part, os, wo):
    r, d = x.shape
    hw = os[0].shape[1]
    nt = 512

    def body(me_ref, x_ref, p_ref, o0, o1, o2, o3, w_ref, y_ref):
        acc = None
        for k, o_ref in enumerate((o0, o1, o2, o3)):
            rows = pl.ds(pl.multiple_of((me_ref[0] ^ k) * hw, hw), hw)
            t = _dot(o_ref[...], w_ref[rows, :])
            acc = t if acc is None else acc + t
        y_ref[...] = (x_ref[...].astype(F32) + acc + p_ref[...]).astype(BF16)

    tile = pl.BlockSpec((r, nt), lambda j, m: (0, j))
    whole = pl.BlockSpec((r, hw), lambda j, m: (0, 0))
    return pl.pallas_call(
        body,
        grid_spec=pltpu.PrefetchScalarGridSpec(
            num_scalar_prefetch=1, grid=(d // nt,),
            in_specs=[tile, tile, whole, whole, whole, whole,
                      pl.BlockSpec((4 * hw, nt), lambda j, m: (0, j))],
            out_specs=tile),
        out_shape=jax.ShapeDtypeStruct((r, d), BF16), compiler_params=_params(1), name="final",
        cost_estimate=_cost(2 * r * d * 4 * hw, 2 * d * 4 * hw + 8 * r * d),
    )(me, x, part, *os, wo)


def solution(mesh):
    nseq = mesh.shape["seq"]

    def swap(t, k):
        return lax.ppermute(t, "seq", [(i, i ^ k) for i in range(nseq)])

    def local(x, g1, b1, g2, b2, wqkv, wo, w1, w2):
        nh, dh, d = wo.shape
        r = x.shape[0]
        me = lax.axis_index("seq").astype(jnp.int32)[None]
        h, qkv = _front(x, g1, b1, g2, b2, _rope_tables(nseq * r, dh), wqkv, w1)
        os = _attention(me, qkv, dh)
        os = [os[0]] + [swap(os[k], k) for k in range(1, nseq)]
        part = _mlp2(h, w2)
        return _final(me, x, part, os, wo.reshape(nh * dh, d))

    rows = P(("data", "seq"), None)
    rep = P()
    return jax.shard_map(local, mesh=mesh,
                         in_specs=(rows, rep, rep, rep, rep, rep, rep, rep, rep),
                         out_specs=rows, check_vma=False)
```

```python
import functools

import jax
import jax.numpy as jnp
from jax import lax
from jax.experimental import pallas as pl
from jax.experimental.pallas import tpu as pltpu
from jax.sharding import PartitionSpec as P

EPS = 1e-5
NEG = -1e30
F32 = jnp.float32
BF16 = jnp.bfloat16
VMEM = 60 * 1024 * 1024


def _cost(flops, nbytes):
    return pl.CostEstimate(flops=int(flops), bytes_accessed=int(nbytes), transcendentals=0)


def _dot(a, b):
    return jnp.dot(a, b, preferred_element_type=F32)


MESH = pl.DeviceIdType.MESH
LO = 64


def _rope_tables(s, dh):
    half = dh // 2
    e = lax.broadcasted_iota(jnp.int32, (1, dh), 1)
    inv = 10000.0 ** (-2.0 * (e % half).astype(F32) / dh)
    lo = jnp.arange(LO).astype(F32)[:, None] * inv
    hi = (LO * jnp.arange(s // LO)).astype(F32)[:, None] * inv
    return jnp.cos(lo), jnp.sin(lo), jnp.cos(hi), jnp.sin(hi)


def _front(x, g1, b1, g2, b2, tabs, wqkv, w1):
    r, d = x.shape
    f = w1.shape[1]
    w3 = wqkv.shape[1] // 3
    hw = w3 // 4
    dh = tabs[0].shape[1]
    nt = 512
    mt = 2 * nt
    cw = 256
    t1 = f // mt
    nb = hw // nt
    t2 = 3 * nb
    ntile1 = f // nt
    ntiles = ntile1 + 2 * t2
    ring = 5
    xc = 128
    steps = t1 + 2 * t2 + 1

    def body(x_ref, g1_ref, b1_ref, g2_ref, b2_ref, cl, sl, ch, sh, wqkv_ref, w1_ref,
             h_ref, qkv_ref, x_scr, rows, m_scr, w_scr, t_scr, cos_s, sin_s,
             xsem, wsem, send, recv):
        s = pl.program_id(0)
        me = lax.axis_index("seq")
        core = me % 2
        near = me + 1 - 2 * core
        far = (me + 2) % 4

        def member(k):
            return [me, near, far, 3 - me][k]

        def load(i):
            slot = i % ring

            @pl.when(i < ntile1)
            def _():
                c = pl.multiple_of(i * nt, nt)
                pltpu.make_async_copy(w1_ref.at[:, pl.ds(c, nt)], w_scr.at[slot], wsem.at[slot]).start()

            @pl.when((i >= ntile1) & (i < ntiles))
            def _():
                v = (i - ntile1) % t2
                c = pl.multiple_of((v // nb) * w3 + me * hw + (v % nb) * nt, nt)
                pltpu.make_async_copy(wqkv_ref.at[:, pl.ds(c, nt)], w_scr.at[slot], wsem.at[slot]).start()

        def ready(i):
            slot = i % ring
            pltpu.make_async_copy(w1_ref.at[:, pl.ds(0, nt)], w_scr.at[slot], wsem.at[slot]).wait()
            return slot

        def remote(src, dst, part, sem, dev):
            return pltpu.make_async_remote_copy(
                src_ref=rows.at[src, part], dst_ref=rows.at[dst, part], send_sem=send.at[sem],
                recv_sem=recv.at[sem], device_id={"seq": dev}, device_id_type=MESH)

        def to_near():
            return remote(0, 1, pl.ds(0, r), 0, near)

        def to_far(p):
            return remote(0, 2, pl.ds(p * (r // 2), r // 2), 1 + p, far)

        def onward(p):
            return remote(2, 3, pl.ds(p * (r // 2), r // 2), 3 + p, near)

        def norm(c, q, _):
            base = c * xc + q * 32
            groups = [pl.ds(pl.multiple_of(base + 16 * g, 16), 16) for g in range(2)]
            nl = d // 128

            def col(rs, j):
                return x_scr[rs, j * 128:(j + 1) * 128].astype(F32)

            def total(f):
                part = [[None] * 4 for _ in groups]
                for j in range(nl):
                    for g, rs in enumerate(groups):
                        v = f(g, col(rs, j))
                        part[g][j % 4] = v if part[g][j % 4] is None else part[g][j % 4] + v
                return [jnp.sum((p[0] + p[1]) + (p[2] + p[3]), axis=-1, keepdims=True) / d for p in part]

            mu = total(lambda g, v: v)
            var = total(lambda g, v: (v - mu[g]) * (v - mu[g]))
            rs_ = [lax.rsqrt(v + EPS) for v in var]
            for j in range(nl):
                cs = slice(j * 128, (j + 1) * 128)
                for g, rs in enumerate(groups):
                    xn = (col(rs, j) - mu[g]) * rs_[g]
                    rows[0, rs, cs] = (xn * g1_ref[:, cs] + b1_ref[:, cs]).astype(BF16)
                    m_scr[rs, cs] = (xn * g2_ref[:, cs] + b2_ref[:, cs]).astype(BF16)
            return 0

        @pl.when(s == 0)
        def _():
            def chunk(c):
                rs = pl.ds(c * xc, xc)
                return pltpu.make_async_copy(x_ref.at[rs], x_scr.at[rs], xsem.at[c])

            for c in range(r // xc):
                chunk(c).start()
            for i in range(ring):
                load(i)
            bar = pltpu.get_barrier_semaphore()
            for dev in (near, far):
                pl.semaphore_signal(bar, inc=1, device_id={"seq": dev}, device_id_type=MESH)
            for c in range(r // xc):
                chunk(c).wait()

                lax.fori_loop(0, xc // 32, functools.partial(norm, c), 0)
                if c == r // xc // 2 - 1:
                    pl.semaphore_wait(bar, 2)
                    to_far(0).start()
            to_far(1).start()
            to_near().start()
            neg = lax.broadcasted_iota(jnp.int32, (LO, dh), 1) < dh // 2
            for k in range(4):
                n = r // LO
                base = pl.ds(pl.multiple_of(member(k) * n, n), n)
                hc, hs = ch[base, :], sh[base, :]
                for i in range(n):
                    a, b = hc[i:i + 1], hs[i:i + 1]
                    sn = b * cl[...] + a * sl[...]
                    cos_s[k, i * LO:(i + 1) * LO, :] = a * cl[...] - b * sl[...]
                    sin_s[k, i * LO:(i + 1) * LO, :] = jnp.where(neg, -sn, sn)

        def gelu(cols):
            t = t_scr[:, cols]
            h_ref[:, cols] = (0.5 * t * (1.0 + lax.erf(t * (0.5 ** 0.5)))).astype(BF16)

        def mlp(first):
            slots = [ready(2 * s + half) for half in range(mt // nt)]
            for half, slot in enumerate(slots):
                for c in range(nt // cw):
                    cols = slice(half * nt + c * cw, half * nt + (c + 1) * cw)
                    if not first:
                        gelu(cols)
                    t_scr[:, cols] = _dot(m_scr[...], w_scr[slot, :, c * cw:(c + 1) * cw])
            load(2 * s + ring)
            load(2 * s + ring + 1)

        pl.when(s == 0)(lambda: mlp(True))
        pl.when((s > 0) & (s < t1))(lambda: mlp(False))

        def rope(j):
            u = s - 1 - t1
            isv = (u % t2) // nb == 2
            base = 2 * (u // t2)
            k, c = j // (nt // cw), j % (nt // cw)
            out = pl.ds(pl.multiple_of((core if k == 0 else 1 - core) * r, r), r)
            t = t_scr[:, j * cw:(j + 1) * cw].astype(BF16).astype(F32)
            for hd in range(cw // dh):
                p = t[:, hd * dh:(hd + 1) * dh]
                v = p * cos_s[base + k] + pltpu.roll(p, dh // 2, 1) * sin_s[base + k]
                lo = c * cw + hd * dh
                qkv_ref[out, lo:lo + dh] = jnp.where(isv, p, v).astype(BF16)

        def qkv(first):
            u = s - t1
            slot = ready(ntile1 + u)
            base = 2 * (u // t2)
            for j in range(mt // cw):
                cols = slice(j * cw, (j + 1) * cw)
                k, c = j // (nt // cw), j % (nt // cw)
                if first:
                    gelu(cols)
                else:
                    rope(j)
                t_scr[:, cols] = _dot(rows[base + k], w_scr[slot, :, c * cw:(c + 1) * cw])
            load(ntile1 + u + ring)

        @pl.when(s == t1)
        def _():
            to_near().wait_recv()
            to_far(0).wait_recv()
            onward(0).start()
            qkv(True)

        @pl.when(s == t1 + t2 - 2)
        def _():
            to_far(1).wait_recv()
            onward(1).start()

        @pl.when(s == t1 + t2)
        def _():
            onward(0).wait_recv()
            onward(1).wait_recv()

        pl.when((s > t1) & (s < steps - 1))(lambda: qkv(False))

        @pl.when(s == steps - 1)
        def _():
            for j in range(mt // cw):
                rope(j)

        @pl.when(s == steps - 1)
        def _():
            to_near().wait_send()
            for p in range(2):
                to_far(p).wait_send()
                onward(p).wait_send()

    def h_map(s):
        return 0, jnp.clip(s - 1, 0, t1 - 1)

    def qkv_map(s):
        u = jnp.maximum(s - 1 - t1, 0)
        chip = lax.axis_index("seq") // 2
        second = u // t2
        return chip + second * (1 - 2 * chip), u % t2

    def full(shape):
        return pl.BlockSpec(shape, lambda s: (0, 0))

    anyspace = pl.BlockSpec(memory_space=pl.ANY)
    return pl.pallas_call(
        body,
        grid=(steps,),
        in_specs=[anyspace] + [full((1, d))] * 4 + [full(t.shape) for t in tabs] + [anyspace] * 2,
        out_specs=[pl.BlockSpec((r, mt), h_map), pl.BlockSpec((2 * r, nt), qkv_map)],
        out_shape=[jax.ShapeDtypeStruct((r, f), BF16), jax.ShapeDtypeStruct((4 * r, 3 * hw), BF16)],
        scratch_shapes=[
            pltpu.VMEM((r, d), BF16), pltpu.VMEM((4, r, d), BF16), pltpu.VMEM((r, d), BF16), pltpu.VMEM((ring, d, nt), BF16),
            pltpu.VMEM((r, mt), F32), pltpu.VMEM((4, r, dh), F32), pltpu.VMEM((4, r, dh), F32),
            pltpu.SemaphoreType.DMA((r // xc,)), pltpu.SemaphoreType.DMA((ring,)),
            pltpu.SemaphoreType.DMA((5,)), pltpu.SemaphoreType.DMA((5,))],
        compiler_params=pltpu.CompilerParams(
            dimension_semantics=("arbitrary",), vmem_limit_bytes=VMEM, collective_id=0,
            has_side_effects=True),
        name="front",
        cost_estimate=_cost(2 * r * d * f + 2 * 4 * r * d * 3 * hw, 2 * d * f + 4 * d * 3 * hw),
    )(x, g1[None], b1[None], g2[None], b2[None], *tabs, wqkv, w1)


def _back(x, qkv, h, w2, wo, dh):
    r, d = x.shape
    s, w = qkv.shape
    f = h.shape[1]
    hw = w // 3
    nh = hw // dh
    qb = 256
    c2 = dh ** -0.5 * 1.4426950408889634
    nblk = s // qb
    nt = 512
    cw = 256
    ck = 4096
    nk = f // ck
    nn = d // nt
    ring = 4
    ta, tw, to = nh, nn * nk // 2, nn // 2
    steps = ta + tw + to
    ntile2 = nn * nk
    ntiles = ntile2 + nn

    def body(x_ref, q_ref, k_ref, v_ref, h_ref, w2_ref, wo_ref, y_ref,
             kt, vx, pb, o_scr, o_send, o_all, h_scr, w_scr, acc, hsem, wsem, send, recv):
        step = pl.program_id(0)
        me = lax.axis_index("seq")
        near = me + 1 - 2 * (me % 2)
        members = [me, near, (me + 2) % 4, 3 - me]

        def load(i):
            slot = i % ring

            @pl.when(i < ntile2)
            def _():
                rows = pl.ds(pl.multiple_of((i % nk) * ck, ck), ck)
                cols = pl.ds(pl.multiple_of((i // nk) * nt, nt), nt)
                pltpu.make_async_copy(w2_ref.at[rows, cols], w_scr.at[slot], wsem.at[slot]).start()

            @pl.when((i >= ntile2) & (i < ntiles))
            def _():
                cols = pl.ds(pl.multiple_of((i - ntile2) * nt, nt), nt)
                pltpu.make_async_copy(wo_ref.at[:, cols], w_scr.at[slot], wsem.at[slot]).start()

        def ready(i):
            slot = i % ring
            pltpu.make_async_copy(wo_ref.at[:, pl.ds(0, nt)], w_scr.at[slot], wsem.at[slot]).wait()
            return slot

        def hcopy(c):
            return pltpu.make_async_copy(h_ref.at[:, pl.ds(c * ck, ck)], h_scr.at[c], hsem.at[c])

        def share(k):
            return pltpu.make_async_remote_copy(
                src_ref=o_send.at[k - 1],
                dst_ref=o_all.at[:, pl.ds(pl.multiple_of(me * hw, hw), hw)],
                send_sem=send.at[k - 1], recv_sem=recv.at[k - 1],
                device_id={"seq": members[k]}, device_id_type=MESH)

        for c in range(nk):
            @pl.when(step == c)
            def _(c=c):
                hcopy(c).start()

        for i in range(ring):
            @pl.when(step == ta - ring + i)
            def _(i=i):
                load(i)

        bar = pltpu.get_barrier_semaphore()

        @pl.when(step == 0)
        def _():
            for k in range(1, 4):
                pl.semaphore_signal(bar, inc=1, device_id={"seq": members[k]}, device_id_type=MESH)
            vx[:, dh:] = jnp.ones((s, dh), BF16)

        row = lax.broadcasted_iota(jnp.int32, (qb, qb), 0)
        col = lax.broadcasted_iota(jnp.int32, (qb, qb), 1)
        keep = col <= row

        def scores(b):
            q = q_ref[b * qb:(b + 1) * qb, :]
            m = None
            for c in range(b + 1):
                cols = slice(c * qb, (c + 1) * qb)
                t = _dot(q, kt[:, cols])
                if c == b:
                    t = jnp.where(keep, t, NEG)
                acc[(b % 2) * (s // nt) + c * qb // nt, :qb, (c * qb) % nt:(c * qb) % nt + qb] = t
                for g in range(qb // dh):
                    u = t[:, g * dh:(g + 1) * dh]
                    m = u if m is None else jnp.maximum(m, u)
            return jnp.max(m, axis=-1, keepdims=True) * c2

        def finish(b, m):
            n = (b + 1) * qb
            for c in range(b + 1):
                t = acc[(b % 2) * (s // nt) + c * qb // nt, :qb, (c * qb) % nt:(c * qb) % nt + qb]
                pb[b % 2, :, c * qb:(c + 1) * qb] = jnp.exp2(t * c2 - m).astype(BF16)
            o = _dot(pb[b % 2, :, :n], vx[:n, :])
            o_scr[b * qb:n, :] = (o[:, :dh] / o[:, dh:]).astype(BF16)

        @pl.when(step < ta)
        def _():
            for c in range(nblk):
                cols = slice(c * qb, (c + 1) * qb)
                vx[cols, :dh] = v_ref[cols, :]
                kt[:, cols] = k_ref[cols, :].T
            m = scores(0)
            for b in range(nblk):
                ahead = scores(b + 1) if b + 1 < nblk else None
                finish(b, m)
                m = ahead
            own = pl.ds(pl.multiple_of(me * r, r), r)
            lanes = pl.ds(pl.multiple_of(step * dh, dh), dh)
            o_all[:, pl.ds(pl.multiple_of(me * hw + step * dh, dh), dh)] = o_scr[own, :]
            for k in range(1, 4):
                o_send[k - 1, :, lanes] = o_scr[pl.ds(pl.multiple_of(members[k] * r, r), r), :]

        @pl.when(step == ta)
        def _():
            pl.semaphore_wait(bar, 3)
            for k in (2, 3, 1):
                share(k).start()
            for c in range(nk // 2):
                hcopy(c).wait()

        @pl.when(step == ta + 1)
        def _():
            for c in range(nk // 2, nk):
                hcopy(c).wait()

        u = step - ta

        def second(first):
            slots = [ready(2 * u), ready(2 * u + 1)]
            kc = 2 * (u % 2)
            for c in range(nt // cw):
                cols = slice(c * cw, (c + 1) * cw)
                t = _dot(h_scr[kc], w_scr[slots[0], :, cols]) + _dot(h_scr[kc + 1], w_scr[slots[1], :, cols])
                acc[u // 2, :, cols] = t if first else acc[u // 2, :, cols] + t
            load(2 * u + ring)
            load(2 * u + ring + 1)

        pl.when((u >= 0) & (u < tw) & (u % 2 == 0))(lambda: second(True))
        pl.when((u >= 0) & (u < tw) & (u % 2 == 1))(lambda: second(False))

        @pl.when(u == tw)
        def _():
            for k in range(1, 4):
                share(k).wait_recv()

        @pl.when(u >= tw)
        def _():
            slots = [ready(2 * u), ready(2 * u + 1)]
            for half, slot in enumerate(slots):
                for c in range(nt // cw):
                    cols = slice(c * cw, (c + 1) * cw)
                    out = slice(half * nt + c * cw, half * nt + (c + 1) * cw)
                    t = _dot(o_all[...], w_scr[slot, :, cols])
                    t = (x_ref[:, out].astype(F32) + t) + acc[2 * (u - tw) + half, :, cols]
                    y_ref[:, out] = t.astype(BF16)
            load(2 * u + ring)
            load(2 * u + ring + 1)

        @pl.when(step == steps - 1)
        def _():
            for k in range(1, 4):
                share(k).wait_send()

    def col(base):
        return pl.BlockSpec((s, dh), lambda i: (0, base + jnp.minimum(i, nh - 1)))

    tile = pl.BlockSpec((r, 2 * nt), lambda i: (0, jnp.clip(i - ta - tw, 0, to - 1)))
    anyspace = pl.BlockSpec(memory_space=pl.ANY)
    return pl.pallas_call(
        body,
        grid=(steps,),
        in_specs=[tile, col(0), col(nh), col(2 * nh)] + [anyspace] * 3,
        out_specs=tile,
        out_shape=jax.ShapeDtypeStruct((r, d), BF16),
        scratch_shapes=[
            pltpu.VMEM((dh, s), BF16), pltpu.VMEM((s, 2 * dh), BF16), pltpu.VMEM((2, qb, s), BF16),
            pltpu.VMEM((s, dh), BF16), pltpu.VMEM((3, r, hw), BF16), pltpu.VMEM((r, 4 * hw), BF16),
            pltpu.VMEM((nk, r, ck), BF16), pltpu.VMEM((ring, ck, nt), BF16), pltpu.VMEM((nn, r, nt), F32),
            pltpu.SemaphoreType.DMA((nk,)), pltpu.SemaphoreType.DMA((ring,)),
            pltpu.SemaphoreType.DMA((3,)), pltpu.SemaphoreType.DMA((3,))],
        compiler_params=pltpu.CompilerParams(
            dimension_semantics=("arbitrary",), vmem_limit_bytes=63 * 1024 * 1024, collective_id=1,
            has_side_effects=True),
        name="back",
        cost_estimate=_cost(4 * s * s * dh * nh + 2 * r * d * (f + 4 * hw), 2 * d * (f + 4 * hw)),
    )(x, qkv, qkv, qkv, h, w2, wo)


def solution(mesh):
    nseq = mesh.shape["seq"]

    def local(x, g1, b1, g2, b2, wqkv, wo, w1, w2):
        nh, dh, d = wo.shape
        r = x.shape[0]
        h, qkv = _front(x, g1, b1, g2, b2, _rope_tables(nseq * r, dh), wqkv, w1)
        return _back(x, qkv, h, w2, wo.reshape(nh * dh, d), dh)

    rows = P(("data", "seq"), None)
    rep = P()
    return jax.shard_map(local, mesh=mesh,
                         in_specs=(rows, rep, rep, rep, rep, rep, rep, rep, rep),
                         out_specs=rows, check_vma=False)
```

```python
import functools

import jax
import jax.numpy as jnp
from jax import lax
from jax.experimental import pallas as pl
from jax.experimental.pallas import tpu as pltpu
from jax.sharding import PartitionSpec as P

EPS = 1e-5
NEG = -1e30
F32 = jnp.float32
BF16 = jnp.bfloat16
VMEM = 60 * 1024 * 1024


def _cost(flops, nbytes):
    return pl.CostEstimate(flops=int(flops), bytes_accessed=int(nbytes), transcendentals=0)


def _dot(a, b):
    return jnp.dot(a, b, preferred_element_type=F32)


MESH = pl.DeviceIdType.MESH
LO = 64


def _rope_angles(s, dh):
    half = dh // 2
    e = lax.broadcasted_iota(jnp.int32, (1, dh), 1)
    inv = 10000.0 ** (-2.0 * (e % half).astype(F32) / dh)
    lo = jnp.arange(LO).astype(F32)[:, None] * inv
    hi = (LO * jnp.arange(s // LO)).astype(F32)[:, None] * inv
    return lo, hi


def _front(x, g1, b1, g2, b2, angles, wqkv, w1):
    r, d = x.shape
    f = w1.shape[1]
    w3 = wqkv.shape[1] // 3
    hw = w3 // 4
    dh = angles[0].shape[1]
    nt = 512
    mt = 2 * nt
    cw = 256
    t1 = f // mt
    nb = hw // nt
    t2 = 3 * nb
    ntile1 = f // nt
    ring = 5
    xc = 128

    def body(x_ref, g1_ref, b1_ref, g2_ref, b2_ref, lo_ref, hi_ref, wqkv_ref, w1_ref,
             h_ref, qkv_ref, x_scr, rows, m_scr, w_scr, t_scr, cos_s, sin_s, h_buf, q_buf,
             xsem, wsem, hsem, qsem, send, recv):
        me = lax.axis_index("seq")
        core = me % 2
        near = me + 1 - 2 * core
        far = (me + 2) % 4

        def member(k):
            return [me, near, far, 3 - me][k]

        def load1(i):
            c = pl.multiple_of(i * nt, nt)
            pltpu.make_async_copy(w1_ref.at[:, pl.ds(c, nt)], w_scr.at[i % ring], wsem.at[i % ring]).start()

        def load2(i):
            slot = (i + ntile1) % ring
            v = i % t2
            c = pl.multiple_of((v // nb) * w3 + me * hw + (v % nb) * nt, nt)
            pltpu.make_async_copy(wqkv_ref.at[:, pl.ds(c, nt)], w_scr.at[slot], wsem.at[slot]).start()

        def ready(i):
            slot = i % ring
            pltpu.make_async_copy(w1_ref.at[:, pl.ds(0, nt)], w_scr.at[slot], wsem.at[slot]).wait()
            return slot

        def remote(src, dst, part, sem, dev):
            return pltpu.make_async_remote_copy(
                src_ref=rows.at[src, part], dst_ref=rows.at[dst, part], send_sem=send.at[sem],
                recv_sem=recv.at[sem], device_id={"seq": dev}, device_id_type=MESH)

        def to_near():
            return remote(0, 1, pl.ds(0, r), 0, near)

        def to_far(p):
            return remote(0, 2, pl.ds(p * (r // 2), r // 2), 1 + p, far)

        def onward(p):
            return remote(2, 3, pl.ds(p * (r // 2), r // 2), 3 + p, near)

        def norm(c, q, _):
            base = c * xc + q * 32
            groups = [pl.ds(pl.multiple_of(base + 16 * g, 16), 16) for g in range(2)]
            nl = d // 128

            def col(rs, j):
                return x_scr[rs, j * 128:(j + 1) * 128].astype(F32)

            def total(f):
                part = [[None] * 4 for _ in groups]
                for j in range(nl):
                    for g, rs in enumerate(groups):
                        v = f(g, col(rs, j))
                        part[g][j % 4] = v if part[g][j % 4] is None else part[g][j % 4] + v
                return [jnp.sum((p[0] + p[1]) + (p[2] + p[3]), axis=-1, keepdims=True) / d for p in part]

            mu = total(lambda g, v: v)
            var = total(lambda g, v: (v - mu[g]) * (v - mu[g]))
            rs_ = [lax.rsqrt(v + EPS) for v in var]
            for j in range(nl):
                cs = slice(j * 128, (j + 1) * 128)
                for g, rs in enumerate(groups):
                    xn = (col(rs, j) - mu[g]) * rs_[g]
                    rows[0, rs, cs] = (xn * g1_ref[:, cs] + b1_ref[:, cs]).astype(BF16)
                    m_scr[rs, cs] = (xn * g2_ref[:, cs] + b2_ref[:, cs]).astype(BF16)
            return 0

        def chunk(c):
            rs = pl.ds(c * xc, xc)
            return pltpu.make_async_copy(x_ref.at[rs], x_scr.at[rs], xsem.at[c])

        for c in range(r // xc):
            chunk(c).start()
        for i in range(ring):
            load1(i)
        bar = pltpu.get_barrier_semaphore()
        for dev in (near, far):
            pl.semaphore_signal(bar, inc=1, device_id={"seq": dev}, device_id_type=MESH)
        neg = lax.broadcasted_iota(jnp.int32, (LO, dh), 1) < dh // 2
        cl, sl = jnp.cos(lo_ref[...]), jnp.sin(lo_ref[...])
        cos_s[0, :hi_ref.shape[0], :] = jnp.cos(hi_ref[...])
        sin_s[0, :hi_ref.shape[0], :] = jnp.sin(hi_ref[...])
        n = r // LO
        highs = []
        for k in range(4):
            base = pl.ds(pl.multiple_of(member(k) * n, n), n)
            highs.append((cos_s[0, base, :], sin_s[0, base, :]))
        for k, (hc, hs) in enumerate(highs):
            for i in range(n):
                a, b = hc[i:i + 1], hs[i:i + 1]
                sn = b * cl + a * sl
                cos_s[k, i * LO:(i + 1) * LO, :] = a * cl - b * sl
                sin_s[k, i * LO:(i + 1) * LO, :] = jnp.where(neg, -sn, sn)
        for c in range(r // xc):
            chunk(c).wait()
            lax.fori_loop(0, xc // 32, functools.partial(norm, c), 0)
            if c == r // xc // 2 - 1:
                pl.semaphore_wait(bar, 2)
                to_far(0).start()
        to_far(1).start()
        to_near().start()

        def h_out(i):
            c = pl.multiple_of(i * mt, mt)
            return pltpu.make_async_copy(h_buf.at[i % 2], h_ref.at[:, pl.ds(c, mt)], hsem.at[i % 2])

        def q_out(i):
            v = i % t2
            chip = me // 2
            pair = chip + (i // t2) * (1 - 2 * chip)
            rs = pl.ds(pl.multiple_of(pair * 2 * r, 2 * r), 2 * r)
            c = pl.multiple_of(v * nt, nt)
            return pltpu.make_async_copy(q_buf.at[i % 2], qkv_ref.at[rs, pl.ds(c, nt)], qsem.at[i % 2])


        def gelu(i, cols):
            t = t_scr[:, cols]
            h_buf[i % 2, :, cols] = (0.5 * t * (1.0 + lax.erf(t * (0.5 ** 0.5)))).astype(BF16)

        def mlp(s, first):
            slots = [ready(2 * s + half) for half in range(mt // nt)]
            for half, slot in enumerate(slots):
                for c in range(nt // cw):
                    cols = slice(half * nt + c * cw, half * nt + (c + 1) * cw)
                    if not first:
                        gelu(s - 1, cols)
                    t_scr[:, cols] = _dot(m_scr[...], w_scr[slot, :, c * cw:(c + 1) * cw])
            if not first:
                h_out(s - 1).start()

        def rope(i, j):
            isv = (i % t2) // nb == 2
            base = 2 * (i // t2)
            k, c = j // (nt // cw), j % (nt // cw)
            out = pl.ds(pl.multiple_of((core if k == 0 else 1 - core) * r, r), r)
            t = t_scr[:, j * cw:(j + 1) * cw].astype(BF16).astype(F32)
            for hd in range(cw // dh):
                p = t[:, hd * dh:(hd + 1) * dh]
                v = p * cos_s[base + k] + pltpu.roll(p, dh // 2, 1) * sin_s[base + k]
                lo = c * cw + hd * dh
                q_buf[i % 2, out, lo:lo + dh] = jnp.where(isv, p, v).astype(BF16)

        def qkv(u, first):
            slot = ready(ntile1 + u)
            base = 2 * (u // t2)
            for j in range(mt // cw):
                cols = slice(j * cw, (j + 1) * cw)
                k, c = j // (nt // cw), j % (nt // cw)
                if first:
                    gelu(t1 - 1, cols)
                else:
                    rope(u - 1, j)
                t_scr[:, cols] = _dot(rows[base + k], w_scr[slot, :, c * cw:(c + 1) * cw])

        mlp(0, True)
        load1(ring)
        load1(ring + 1)

        inner = (ntile1 - ring - 2) // 2 + 1

        def mlp_step(s, _):
            @pl.when(s > 2)
            def _():
                h_out(s - 3).wait()

            mlp(s, False)

            @pl.when(s < inner)
            def _():
                load1(2 * s + ring)
                load1(2 * s + ring + 1)

            @pl.when(s >= inner)
            def _():
                i = 2 * s + ring

                @pl.when(i < ntile1)
                def _():
                    load1(i)

                @pl.when(i >= ntile1)
                def _():
                    load2(i - ntile1)

                load2(i + 1 - ntile1)
            return 0

        lax.fori_loop(1, t1, mlp_step, 0)

        to_near().wait_recv()
        to_far(0).wait_recv()
        onward(0).start()
        h_out(t1 - 3).wait()
        qkv(0, True)
        h_out(t1 - 1).start()
        load2(ring)

        def qkv_step(u, _):
            @pl.when(u == t2 - 2)
            def _():
                to_far(1).wait_recv()
                onward(1).start()

            @pl.when(u == t2)
            def _():
                onward(0).wait_recv()
                onward(1).wait_recv()

            @pl.when(u > 2)
            def _():
                q_out(u - 3).wait()

            qkv(u, False)
            q_out(u - 1).start()

            @pl.when(u + ring < 2 * t2)
            def _():
                load2(u + ring)
            return 0

        lax.fori_loop(1, 2 * t2, qkv_step, 0)
        q_out(2 * t2 - 3).wait()
        for j in range(mt // cw):
            rope(2 * t2 - 1, j)
        q_out(2 * t2 - 1).start()
        h_out(t1 - 2).wait()
        h_out(t1 - 1).wait()
        q_out(2 * t2 - 2).wait()
        q_out(2 * t2 - 1).wait()
        to_near().wait_send()
        for p in range(2):
            to_far(p).wait_send()
            onward(p).wait_send()

    anyspace = pl.BlockSpec(memory_space=pl.ANY)
    inside = pl.BlockSpec(memory_space=pltpu.VMEM)
    return pl.pallas_call(
        body,
        in_specs=[anyspace] + [inside] * 6 + [anyspace] * 2,
        out_specs=[anyspace, anyspace],
        out_shape=[jax.ShapeDtypeStruct((r, f), BF16), jax.ShapeDtypeStruct((4 * r, 3 * hw), BF16)],
        scratch_shapes=[
            pltpu.VMEM((r, d), BF16), pltpu.VMEM((4, r, d), BF16), pltpu.VMEM((r, d), BF16),
            pltpu.VMEM((ring, d, nt), BF16),
            pltpu.VMEM((r, mt), F32), pltpu.VMEM((4, r, dh), F32), pltpu.VMEM((4, r, dh), F32),
            pltpu.VMEM((2, r, mt), BF16), pltpu.VMEM((2, 2 * r, nt), BF16),
            pltpu.SemaphoreType.DMA((r // xc,)), pltpu.SemaphoreType.DMA((ring,)),
            pltpu.SemaphoreType.DMA((2,)), pltpu.SemaphoreType.DMA((2,)),
            pltpu.SemaphoreType.DMA((5,)), pltpu.SemaphoreType.DMA((5,))],
        compiler_params=pltpu.CompilerParams(
            vmem_limit_bytes=VMEM, collective_id=0, has_side_effects=True),
        name="front",
        cost_estimate=_cost(2 * r * d * f + 2 * 4 * r * d * 3 * hw, 2 * d * f + 4 * d * 3 * hw),
    )(x, g1[None], b1[None], g2[None], b2[None], *angles, wqkv, w1)


def _back(x, qkv, h, w2, wo, dh):
    r, d = x.shape
    s, w = qkv.shape
    f = h.shape[1]
    hw = w // 3
    nh = hw // dh
    qb = 256
    c2 = dh ** -0.5 * 1.4426950408889634
    nblk = s // qb
    nt = 512
    cw = 256
    ck = 4096
    nk = f // ck
    nn = d // nt
    ring = 4
    to = nn // 2
    ntile2 = nn * nk

    def body(x_ref, qkv_ref, h_ref, w2_ref, wo_ref, y_ref,
             qkv_buf, kt, vx, pb, o_scr, o_send, o_all, h_scr, w_scr, acc, x_buf, y_buf,
             asem, hsem, wsem, xsem, ysem, send, recv):
        me = lax.axis_index("seq")
        near = me + 1 - 2 * (me % 2)
        members = [me, near, (me + 2) % 4, 3 - me]

        def load(i, wo=False):
            slot = i % ring
            if wo:
                src = wo_ref.at[:, pl.ds(pl.multiple_of((i - ntile2) * nt, nt), nt)]
            else:
                rows = pl.ds(pl.multiple_of((i % nk) * ck, ck), ck)
                src = w2_ref.at[rows, pl.ds(pl.multiple_of((i // nk) * nt, nt), nt)]
            pltpu.make_async_copy(src, w_scr.at[slot], wsem.at[slot]).start()

        def heads(i):
            return [pltpu.make_async_copy(
                qkv_ref.at[:, pl.ds(pl.multiple_of(t * hw + i * dh, dh), dh)],
                qkv_buf.at[i % 2, t], asem.at[i % 2, t]) for t in range(3)]

        def x_in(i):
            cols = pl.ds(pl.multiple_of(i * 2 * nt, 2 * nt), 2 * nt)
            return pltpu.make_async_copy(x_ref.at[:, cols], x_buf.at[i % 2], xsem.at[i % 2])

        def y_out(i):
            cols = pl.ds(pl.multiple_of(i * 2 * nt, 2 * nt), 2 * nt)
            return pltpu.make_async_copy(y_buf.at[i % 2], y_ref.at[:, cols], ysem.at[i % 2])

        def ready(i):
            slot = i % ring
            pltpu.make_async_copy(wo_ref.at[:, pl.ds(0, nt)], w_scr.at[slot], wsem.at[slot]).wait()
            return slot

        def hcopy(c):
            return pltpu.make_async_copy(h_ref.at[:, pl.ds(c * ck, ck)], h_scr.at[c], hsem.at[c])

        def share(k):
            return pltpu.make_async_remote_copy(
                src_ref=o_send.at[k - 1],
                dst_ref=o_all.at[:, pl.ds(pl.multiple_of(me * hw, hw), hw)],
                send_sem=send.at[k - 1], recv_sem=recv.at[k - 1],
                device_id={"seq": members[k]}, device_id_type=MESH)

        for t in heads(0):
            t.start()
        bar = pltpu.get_barrier_semaphore()
        for k in range(1, 4):
            pl.semaphore_signal(bar, inc=1, device_id={"seq": members[k]}, device_id_type=MESH)
        vx[:, dh:] = jnp.ones((s, dh), BF16)

        row = lax.broadcasted_iota(jnp.int32, (qb, qb), 0)
        col = lax.broadcasted_iota(jnp.int32, (qb, qb), 1)
        keep = col <= row

        def scores(i, b):
            q = qkv_buf[i % 2, 0, b * qb:(b + 1) * qb, :]
            m = None
            for c in range(b + 1):
                cols = slice(c * qb, (c + 1) * qb)
                t = _dot(q, kt[:, cols])
                if c == b:
                    t = jnp.where(keep, t, NEG)
                acc[(b % 2) * (s // nt) + c * qb // nt, :qb, (c * qb) % nt:(c * qb) % nt + qb] = t
                for g in range(qb // dh):
                    u = t[:, g * dh:(g + 1) * dh]
                    m = u if m is None else jnp.maximum(m, u)
            return jnp.max(m, axis=-1, keepdims=True) * c2

        def finish(b, m):
            n = (b + 1) * qb
            for c in range(b + 1):
                t = acc[(b % 2) * (s // nt) + c * qb // nt, :qb, (c * qb) % nt:(c * qb) % nt + qb]
                pb[b % 2, :, c * qb:(c + 1) * qb] = jnp.exp2(t * c2 - m).astype(BF16)
            o = _dot(pb[b % 2, :, :n], vx[:n, :])
            o_scr[b * qb:n, :] = (o[:, :dh] / o[:, dh:]).astype(BF16)

        def head(i, _):
            @pl.when(i + 1 < nh)
            def _():
                for t in heads(i + 1):
                    t.start()

            for c in range(nk):
                @pl.when(i == c)
                def _(c=c):
                    hcopy(c).start()

            for c in range(ring):
                @pl.when(i == nh - ring + c)
                def _(c=c):
                    load(c)

            for t in heads(i):
                t.wait()
            for c in range(nblk):
                cols = slice(c * qb, (c + 1) * qb)
                vx[cols, :dh] = qkv_buf[i % 2, 2, cols, :]
                kt[:, cols] = qkv_buf[i % 2, 1, cols, :].T
            m = scores(i, 0)
            for b in range(nblk):
                ahead = scores(i, b + 1) if b + 1 < nblk else None
                finish(b, m)
                m = ahead
            own = pl.ds(pl.multiple_of(me * r, r), r)
            lanes = pl.ds(pl.multiple_of(i * dh, dh), dh)
            o_all[:, pl.ds(pl.multiple_of(me * hw + i * dh, dh), dh)] = o_scr[own, :]
            for k in range(1, 4):
                o_send[k - 1, :, lanes] = o_scr[pl.ds(pl.multiple_of(members[k] * r, r), r), :]
            return 0

        lax.fori_loop(0, nh, head, 0)
        pl.semaphore_wait(bar, 3)
        for k in (2, 3, 1):
            share(k).start()
        for c in range(nk):
            hcopy(c).wait()

        def second(n, half):
            slots = [ready(nk * n + 2 * half), ready(nk * n + 2 * half + 1)]
            kc = 2 * half
            for c in range(nt // cw):
                cols = slice(c * cw, (c + 1) * cw)
                t = _dot(h_scr[kc], w_scr[slots[0], :, cols]) + _dot(h_scr[kc + 1], w_scr[slots[1], :, cols])
                acc[n, :, cols] = acc[n, :, cols] + t if half else t

        def w2_step(n, _):
            for half in range(nk // 2):
                second(n, half)

                @pl.when(n < nn - 1)
                def _():
                    load(nk * (n + 1) + 2 * half)
                    load(nk * (n + 1) + 2 * half + 1)

                @pl.when(n == nn - 1)
                def _():
                    load(nk * nn + 2 * half, wo=True)
                    load(nk * nn + 2 * half + 1, wo=True)
            return 0

        x_in(0).start()
        lax.fori_loop(0, nn, w2_step, 0)
        for k in range(1, 4):
            share(k).wait_recv()

        def wo_step(n, _):
            @pl.when(n + 1 < to)
            def _():
                x_in(n + 1).start()

            x_in(n).wait()

            @pl.when(n > 1)
            def _():
                y_out(n - 2).wait()

            slots = [ready(ntile2 + 2 * n), ready(ntile2 + 2 * n + 1)]
            for half, slot in enumerate(slots):
                for c in range(nt // cw):
                    cols = slice(c * cw, (c + 1) * cw)
                    out = slice(half * nt + c * cw, half * nt + (c + 1) * cw)
                    t = _dot(o_all[...], w_scr[slot, :, cols])
                    t = (x_buf[n % 2, :, out].astype(F32) + t) + acc[2 * n + half, :, cols]
                    y_buf[n % 2, :, out] = t.astype(BF16)
            y_out(n).start()

            @pl.when(n + 2 < to)
            def _():
                load(ntile2 + 2 * n + ring, wo=True)
                load(ntile2 + 2 * n + ring + 1, wo=True)
            return 0

        lax.fori_loop(0, to, wo_step, 0)
        y_out(to - 2).wait()
        y_out(to - 1).wait()
        for k in range(1, 4):
            share(k).wait_send()

    anyspace = pl.BlockSpec(memory_space=pl.ANY)
    return pl.pallas_call(
        body,
        in_specs=[anyspace] * 5,
        out_specs=anyspace,
        out_shape=jax.ShapeDtypeStruct((r, d), BF16),
        scratch_shapes=[
            pltpu.VMEM((2, 3, s, dh), BF16),
            pltpu.VMEM((dh, s), BF16), pltpu.VMEM((s, 2 * dh), BF16), pltpu.VMEM((2, qb, s), BF16),
            pltpu.VMEM((s, dh), BF16), pltpu.VMEM((3, r, hw), BF16), pltpu.VMEM((r, 4 * hw), BF16),
            pltpu.VMEM((nk, r, ck), BF16), pltpu.VMEM((ring, ck, nt), BF16), pltpu.VMEM((nn, r, nt), F32),
            pltpu.VMEM((2, r, 2 * nt), BF16), pltpu.VMEM((2, r, 2 * nt), BF16),
            pltpu.SemaphoreType.DMA((2, 3)), pltpu.SemaphoreType.DMA((nk,)), pltpu.SemaphoreType.DMA((ring,)),
            pltpu.SemaphoreType.DMA((2,)), pltpu.SemaphoreType.DMA((2,)),
            pltpu.SemaphoreType.DMA((3,)), pltpu.SemaphoreType.DMA((3,))],
        compiler_params=pltpu.CompilerParams(
            vmem_limit_bytes=63 * 1024 * 1024, collective_id=1,
            has_side_effects=True),
        name="back",
        cost_estimate=_cost(4 * s * s * dh * nh + 2 * r * d * (f + 4 * hw), 2 * d * (f + 4 * hw)),
    )(x, qkv, h, w2, wo)


def solution(mesh):
    nseq = mesh.shape["seq"]

    def local(x, g1, b1, g2, b2, wqkv, wo, w1, w2):
        nh, dh, d = wo.shape
        r = x.shape[0]
        h, qkv = _front(x, g1, b1, g2, b2, _rope_angles(nseq * r, dh), wqkv, w1)
        return _back(x, qkv, h, w2, wo.reshape(nh * dh, d), dh)

    rows = P(("data", "seq"), None)
    rep = P()
    return jax.shard_map(local, mesh=mesh,
                         in_specs=(rows, rep, rep, rep, rep, rep, rep, rep, rep),
                         out_specs=rows, check_vma=False)
```

```python
import functools

import jax
import jax.numpy as jnp
import numpy as np
from jax import lax
from jax.experimental import pallas as pl
from jax.experimental.pallas import tpu as pltpu
from jax.sharding import PartitionSpec as P

EPS = 1e-5
NEG = -1e30
F32 = jnp.float32
BF16 = jnp.bfloat16
VMEM = 60 * 1024 * 1024


def _cost(flops, nbytes):
    return pl.CostEstimate(flops=int(flops), bytes_accessed=int(nbytes), transcendentals=0)


def _dot(a, b):
    return jnp.dot(a, b, preferred_element_type=F32)


MESH = pl.DeviceIdType.MESH
LO = 64


def _inverse_frequencies(dh):
    e = np.arange(dh) % (dh // 2)
    return np.asarray(10000.0 ** (-2.0 * e / dh), np.float32)[None]


def _front(x, g1, b1, g2, b2, inv, wqkv, w1):
    r, d = x.shape
    f = w1.shape[1]
    w3 = wqkv.shape[1] // 3
    hw = w3 // 4
    dh = inv.shape[1]
    highs = 4 * r // LO
    nt = 512
    mt = 2 * nt
    cw = 256
    t1 = f // mt
    nb = hw // nt
    t2 = 3 * nb
    ntile1 = f // nt
    ring = 5
    xc = 128

    def body(x_ref, g1_ref, b1_ref, g2_ref, b2_ref, inv_ref, wqkv_ref, w1_ref,
             h_ref, qkv_ref, x_scr, rows, m_scr, w_scr, t_scr, cos_s, sin_s, h_buf, q_buf,
             xsem, wsem, hsem, qsem, send, recv):
        me = lax.axis_index("seq")
        core = me % 2
        near = me + 1 - 2 * core
        far = (me + 2) % 4

        def member(k):
            return [me, near, far, 3 - me][k]

        def load1(i):
            c = pl.multiple_of(i * nt, nt)
            pltpu.make_async_copy(w1_ref.at[:, pl.ds(c, nt)], w_scr.at[i % ring], wsem.at[i % ring]).start()

        def load2(i):
            slot = (i + ntile1) % ring
            v = i % t2
            c = pl.multiple_of((v // nb) * w3 + me * hw + (v % nb) * nt, nt)
            pltpu.make_async_copy(wqkv_ref.at[:, pl.ds(c, nt)], w_scr.at[slot], wsem.at[slot]).start()

        def ready(i):
            slot = i % ring
            pltpu.make_async_copy(w1_ref.at[:, pl.ds(0, nt)], w_scr.at[slot], wsem.at[slot]).wait()
            return slot

        def remote(src, dst, part, sem, dev):
            return pltpu.make_async_remote_copy(
                src_ref=rows.at[src, part], dst_ref=rows.at[dst, part], send_sem=send.at[sem],
                recv_sem=recv.at[sem], device_id={"seq": dev}, device_id_type=MESH)

        def to_near():
            return remote(0, 1, pl.ds(0, r), 0, near)

        def to_far(p):
            return remote(0, 2, pl.ds(p * (r // 2), r // 2), 1 + p, far)

        def onward(p):
            return remote(2, 3, pl.ds(p * (r // 2), r // 2), 3 + p, near)

        def norm(c, q, _):
            base = c * xc + q * 32
            groups = [pl.ds(pl.multiple_of(base + 16 * g, 16), 16) for g in range(2)]
            nl = d // 128

            def col(rs, j):
                return x_scr[rs, j * 128:(j + 1) * 128].astype(F32)

            def total(f):
                part = [[None] * 4 for _ in groups]
                for j in range(nl):
                    for g, rs in enumerate(groups):
                        v = f(g, col(rs, j))
                        part[g][j % 4] = v if part[g][j % 4] is None else part[g][j % 4] + v
                return [jnp.sum((p[0] + p[1]) + (p[2] + p[3]), axis=-1, keepdims=True) / d for p in part]

            mu = total(lambda g, v: v)
            var = total(lambda g, v: (v - mu[g]) * (v - mu[g]))
            rs_ = [lax.rsqrt(v + EPS) for v in var]
            for j in range(nl):
                cs = slice(j * 128, (j + 1) * 128)
                for g, rs in enumerate(groups):
                    xn = (col(rs, j) - mu[g]) * rs_[g]
                    rows[0, rs, cs] = (xn * g1_ref[:, cs] + b1_ref[:, cs]).astype(BF16)
                    m_scr[rs, cs] = (xn * g2_ref[:, cs] + b2_ref[:, cs]).astype(BF16)
            return 0

        def chunk(c):
            rs = pl.ds(c * xc, xc)
            return pltpu.make_async_copy(x_ref.at[rs], x_scr.at[rs], xsem.at[c])

        for c in range(r // xc):
            chunk(c).start()
        for i in range(ring):
            load1(i)
        bar = pltpu.get_barrier_semaphore()
        for dev in (near, far):
            pl.semaphore_signal(bar, inc=1, device_id={"seq": dev}, device_id_type=MESH)
        neg = lax.broadcasted_iota(jnp.int32, (LO, dh), 1) < dh // 2
        lo = lax.broadcasted_iota(jnp.int32, (LO, dh), 0).astype(F32) * inv_ref[...]
        hi = (LO * lax.broadcasted_iota(jnp.int32, (highs, dh), 0)).astype(F32) * inv_ref[...]
        cl, sl = jnp.cos(lo), jnp.sin(lo)
        cos_s[0, :highs, :] = jnp.cos(hi)
        sin_s[0, :highs, :] = jnp.sin(hi)
        n = r // LO
        tables = []
        for k in range(4):
            base = pl.ds(pl.multiple_of(member(k) * n, n), n)
            tables.append((cos_s[0, base, :], sin_s[0, base, :]))
        for k, (hc, hs) in enumerate(tables):
            for i in range(n):
                a, b = hc[i:i + 1], hs[i:i + 1]
                sn = b * cl + a * sl
                cos_s[k, i * LO:(i + 1) * LO, :] = a * cl - b * sl
                sin_s[k, i * LO:(i + 1) * LO, :] = jnp.where(neg, -sn, sn)
        for c in range(r // xc):
            chunk(c).wait()
            lax.fori_loop(0, xc // 32, functools.partial(norm, c), 0)
            if c == r // xc // 2 - 1:
                pl.semaphore_wait(bar, 2)
                to_far(0).start()
        to_far(1).start()
        to_near().start()

        def h_out(i):
            c = pl.multiple_of(i * mt, mt)
            return pltpu.make_async_copy(h_buf.at[i % 2], h_ref.at[:, pl.ds(c, mt)], hsem.at[i % 2])

        def q_out(i):
            v = i % t2
            chip = me // 2
            pair = chip + (i // t2) * (1 - 2 * chip)
            rs = pl.ds(pl.multiple_of(pair * 2 * r, 2 * r), 2 * r)
            c = pl.multiple_of(v * nt, nt)
            return pltpu.make_async_copy(q_buf.at[i % 2], qkv_ref.at[rs, pl.ds(c, nt)], qsem.at[i % 2])


        def gelu(i, cols):
            t = t_scr[:, cols]
            h_buf[i % 2, :, cols] = (0.5 * t * (1.0 + lax.erf(t * (0.5 ** 0.5)))).astype(BF16)

        def mlp(s, first):
            slots = [ready(2 * s + half) for half in range(mt // nt)]
            for half, slot in enumerate(slots):
                for c in range(nt // cw):
                    cols = slice(half * nt + c * cw, half * nt + (c + 1) * cw)
                    if not first:
                        gelu(s - 1, cols)
                    t_scr[:, cols] = _dot(m_scr[...], w_scr[slot, :, c * cw:(c + 1) * cw])
            if not first:
                h_out(s - 1).start()

        def rope(i, j):
            isv = (i % t2) // nb == 2
            base = 2 * (i // t2)
            k, c = j // (nt // cw), j % (nt // cw)
            out = pl.ds(pl.multiple_of((core if k == 0 else 1 - core) * r, r), r)
            t = t_scr[:, j * cw:(j + 1) * cw].astype(BF16).astype(F32)
            for hd in range(cw // dh):
                p = t[:, hd * dh:(hd + 1) * dh]
                v = p * cos_s[base + k] + pltpu.roll(p, dh // 2, 1) * sin_s[base + k]
                lo = c * cw + hd * dh
                q_buf[i % 2, out, lo:lo + dh] = jnp.where(isv, p, v).astype(BF16)

        def qkv(u, first):
            slot = ready(ntile1 + u)
            base = 2 * (u // t2)
            for j in range(mt // cw):
                cols = slice(j * cw, (j + 1) * cw)
                k, c = j // (nt // cw), j % (nt // cw)
                if first:
                    gelu(t1 - 1, cols)
                else:
                    rope(u - 1, j)
                t_scr[:, cols] = _dot(rows[base + k], w_scr[slot, :, c * cw:(c + 1) * cw])

        mlp(0, True)
        load1(ring)
        load1(ring + 1)

        inner = (ntile1 - ring - 2) // 2 + 1

        def mlp_step(s, _):
            @pl.when(s > 2)
            def _():
                h_out(s - 3).wait()

            mlp(s, False)

            @pl.when(s < inner)
            def _():
                load1(2 * s + ring)
                load1(2 * s + ring + 1)

            @pl.when(s >= inner)
            def _():
                i = 2 * s + ring

                @pl.when(i < ntile1)
                def _():
                    load1(i)

                @pl.when(i >= ntile1)
                def _():
                    load2(i - ntile1)

                load2(i + 1 - ntile1)
            return 0

        lax.fori_loop(1, t1, mlp_step, 0)

        to_near().wait_recv()
        to_far(0).wait_recv()
        onward(0).start()
        h_out(t1 - 3).wait()
        qkv(0, True)
        h_out(t1 - 1).start()
        load2(ring)

        def qkv_step(u, _):
            @pl.when(u == t2 - 2)
            def _():
                to_far(1).wait_recv()
                onward(1).start()

            @pl.when(u == t2)
            def _():
                onward(0).wait_recv()
                onward(1).wait_recv()

            @pl.when(u > 2)
            def _():
                q_out(u - 3).wait()

            qkv(u, False)
            q_out(u - 1).start()

            @pl.when(u + ring < 2 * t2)
            def _():
                load2(u + ring)
            return 0

        lax.fori_loop(1, 2 * t2, qkv_step, 0)
        q_out(2 * t2 - 3).wait()
        for j in range(mt // cw):
            rope(2 * t2 - 1, j)
        q_out(2 * t2 - 1).start()
        h_out(t1 - 2).wait()
        h_out(t1 - 1).wait()
        q_out(2 * t2 - 2).wait()
        q_out(2 * t2 - 1).wait()
        to_near().wait_send()
        for p in range(2):
            to_far(p).wait_send()
            onward(p).wait_send()

    anyspace = pl.BlockSpec(memory_space=pl.ANY)
    inside = pl.BlockSpec(memory_space=pltpu.VMEM)
    return pl.pallas_call(
        body,
        in_specs=[anyspace] + [inside] * 5 + [anyspace] * 2,
        out_specs=[anyspace, anyspace],
        out_shape=[jax.ShapeDtypeStruct((r, f), BF16), jax.ShapeDtypeStruct((4 * r, 3 * hw), BF16)],
        scratch_shapes=[
            pltpu.VMEM((r, d), BF16), pltpu.VMEM((4, r, d), BF16), pltpu.VMEM((r, d), BF16),
            pltpu.VMEM((ring, d, nt), BF16),
            pltpu.VMEM((r, mt), F32), pltpu.VMEM((4, r, dh), F32), pltpu.VMEM((4, r, dh), F32),
            pltpu.VMEM((2, r, mt), BF16), pltpu.VMEM((2, 2 * r, nt), BF16),
            pltpu.SemaphoreType.DMA((r // xc,)), pltpu.SemaphoreType.DMA((ring,)),
            pltpu.SemaphoreType.DMA((2,)), pltpu.SemaphoreType.DMA((2,)),
            pltpu.SemaphoreType.DMA((5,)), pltpu.SemaphoreType.DMA((5,))],
        compiler_params=pltpu.CompilerParams(
            vmem_limit_bytes=VMEM, collective_id=0, has_side_effects=True),
        name="front",
        cost_estimate=_cost(2 * r * d * f + 2 * 4 * r * d * 3 * hw, 2 * d * f + 4 * d * 3 * hw),
    )(x, g1[None], b1[None], g2[None], b2[None], inv, wqkv, w1)


def _back(x, qkv, h, w2, wo, dh):
    r, d = x.shape
    s, w = qkv.shape
    f = h.shape[1]
    hw = w // 3
    nh = hw // dh
    qb = 256
    c2 = dh ** -0.5 * 1.4426950408889634
    nblk = s // qb
    nt = 512
    cw = 256
    ck = 4096
    nk = f // ck
    nn = d // nt
    ring = 4
    to = nn // 2
    ntile2 = nn * nk

    def body(x_ref, qkv_ref, h_ref, w2_ref, wo_ref, y_ref,
             qkv_buf, kt, vx, pb, o_scr, o_send, o_all, h_scr, w_scr, acc, x_buf, y_buf,
             asem, hsem, wsem, xsem, ysem, send, recv):
        me = lax.axis_index("seq")
        near = me + 1 - 2 * (me % 2)
        members = [me, near, (me + 2) % 4, 3 - me]

        def load(i, wo=False):
            slot = i % ring
            if wo:
                src = wo_ref.at[:, pl.ds(pl.multiple_of((i - ntile2) * nt, nt), nt)]
            else:
                rows = pl.ds(pl.multiple_of((i % nk) * ck, ck), ck)
                src = w2_ref.at[rows, pl.ds(pl.multiple_of((i // nk) * nt, nt), nt)]
            pltpu.make_async_copy(src, w_scr.at[slot], wsem.at[slot]).start()

        def heads(i):
            return [pltpu.make_async_copy(
                qkv_ref.at[:, pl.ds(pl.multiple_of(t * hw + i * dh, dh), dh)],
                qkv_buf.at[i % 2, t], asem.at[i % 2, t]) for t in range(3)]

        def x_in(i):
            cols = pl.ds(pl.multiple_of(i * 2 * nt, 2 * nt), 2 * nt)
            return pltpu.make_async_copy(x_ref.at[:, cols], x_buf.at[i % 2], xsem.at[i % 2])

        def y_out(i):
            cols = pl.ds(pl.multiple_of(i * 2 * nt, 2 * nt), 2 * nt)
            return pltpu.make_async_copy(y_buf.at[i % 2], y_ref.at[:, cols], ysem.at[i % 2])

        def ready(i):
            slot = i % ring
            pltpu.make_async_copy(wo_ref.at[:, pl.ds(0, nt)], w_scr.at[slot], wsem.at[slot]).wait()
            return slot

        def hcopy(c):
            return pltpu.make_async_copy(h_ref.at[:, pl.ds(c * ck, ck)], h_scr.at[c], hsem.at[c])

        def share(k):
            return pltpu.make_async_remote_copy(
                src_ref=o_send.at[k - 1],
                dst_ref=o_all.at[:, pl.ds(pl.multiple_of(me * hw, hw), hw)],
                send_sem=send.at[k - 1], recv_sem=recv.at[k - 1],
                device_id={"seq": members[k]}, device_id_type=MESH)

        for t in heads(0):
            t.start()
        bar = pltpu.get_barrier_semaphore()
        for k in range(1, 4):
            pl.semaphore_signal(bar, inc=1, device_id={"seq": members[k]}, device_id_type=MESH)
        vx[:, dh:] = jnp.ones((s, dh), BF16)

        row = lax.broadcasted_iota(jnp.int32, (qb, qb), 0)
        col = lax.broadcasted_iota(jnp.int32, (qb, qb), 1)
        keep = col <= row

        def scores(i, b):
            q = qkv_buf[i % 2, 0, b * qb:(b + 1) * qb, :]
            m = None
            for c in range(b + 1):
                cols = slice(c * qb, (c + 1) * qb)
                t = _dot(q, kt[:, cols])
                if c == b:
                    t = jnp.where(keep, t, NEG)
                acc[(b % 2) * (s // nt) + c * qb // nt, :qb, (c * qb) % nt:(c * qb) % nt + qb] = t
                for g in range(qb // dh):
                    u = t[:, g * dh:(g + 1) * dh]
                    m = u if m is None else jnp.maximum(m, u)
            return jnp.max(m, axis=-1, keepdims=True) * c2

        def finish(b, m):
            n = (b + 1) * qb
            for c in range(b + 1):
                t = acc[(b % 2) * (s // nt) + c * qb // nt, :qb, (c * qb) % nt:(c * qb) % nt + qb]
                pb[b % 2, :, c * qb:(c + 1) * qb] = jnp.exp2(t * c2 - m).astype(BF16)
            o = _dot(pb[b % 2, :, :n], vx[:n, :])
            o_scr[b * qb:n, :] = (o[:, :dh] / o[:, dh:]).astype(BF16)

        def head(i, _):
            @pl.when(i + 1 < nh)
            def _():
                for t in heads(i + 1):
                    t.start()

            for c in range(nk):
                @pl.when(i == c)
                def _(c=c):
                    hcopy(c).start()

            for c in range(ring):
                @pl.when(i == nh - ring + c)
                def _(c=c):
                    load(c)

            for t in heads(i):
                t.wait()
            for c in range(nblk):
                cols = slice(c * qb, (c + 1) * qb)
                vx[cols, :dh] = qkv_buf[i % 2, 2, cols, :]
                kt[:, cols] = qkv_buf[i % 2, 1, cols, :].T
            m = scores(i, 0)
            for b in range(nblk):
                ahead = scores(i, b + 1) if b + 1 < nblk else None
                finish(b, m)
                m = ahead
            own = pl.ds(pl.multiple_of(me * r, r), r)
            lanes = pl.ds(pl.multiple_of(i * dh, dh), dh)
            o_all[:, pl.ds(pl.multiple_of(me * hw + i * dh, dh), dh)] = o_scr[own, :]
            for k in range(1, 4):
                o_send[k - 1, :, lanes] = o_scr[pl.ds(pl.multiple_of(members[k] * r, r), r), :]
            return 0

        lax.fori_loop(0, nh, head, 0)
        pl.semaphore_wait(bar, 3)
        for k in (2, 3, 1):
            share(k).start()
        for c in range(nk):
            hcopy(c).wait()

        def second(n, half):
            slots = [ready(nk * n + 2 * half), ready(nk * n + 2 * half + 1)]
            kc = 2 * half
            for c in range(nt // cw):
                cols = slice(c * cw, (c + 1) * cw)
                t = _dot(h_scr[kc], w_scr[slots[0], :, cols]) + _dot(h_scr[kc + 1], w_scr[slots[1], :, cols])
                acc[n, :, cols] = acc[n, :, cols] + t if half else t

        def w2_step(n, _):
            for half in range(nk // 2):
                second(n, half)

                @pl.when(n < nn - 1)
                def _():
                    load(nk * (n + 1) + 2 * half)
                    load(nk * (n + 1) + 2 * half + 1)

                @pl.when(n == nn - 1)
                def _():
                    load(nk * nn + 2 * half, wo=True)
                    load(nk * nn + 2 * half + 1, wo=True)
            return 0

        x_in(0).start()
        lax.fori_loop(0, nn, w2_step, 0)
        for k in range(1, 4):
            share(k).wait_recv()

        def wo_step(n, _):
            @pl.when(n + 1 < to)
            def _():
                x_in(n + 1).start()

            x_in(n).wait()

            @pl.when(n > 1)
            def _():
                y_out(n - 2).wait()

            slots = [ready(ntile2 + 2 * n), ready(ntile2 + 2 * n + 1)]
            for half, slot in enumerate(slots):
                for c in range(nt // cw):
                    cols = slice(c * cw, (c + 1) * cw)
                    out = slice(half * nt + c * cw, half * nt + (c + 1) * cw)
                    t = _dot(o_all[...], w_scr[slot, :, cols])
                    t = (x_buf[n % 2, :, out].astype(F32) + t) + acc[2 * n + half, :, cols]
                    y_buf[n % 2, :, out] = t.astype(BF16)
            y_out(n).start()

            @pl.when(n + 2 < to)
            def _():
                load(ntile2 + 2 * n + ring, wo=True)
                load(ntile2 + 2 * n + ring + 1, wo=True)
            return 0

        lax.fori_loop(0, to, wo_step, 0)
        y_out(to - 2).wait()
        y_out(to - 1).wait()
        for k in range(1, 4):
            share(k).wait_send()

    anyspace = pl.BlockSpec(memory_space=pl.ANY)
    return pl.pallas_call(
        body,
        in_specs=[anyspace] * 5,
        out_specs=anyspace,
        out_shape=jax.ShapeDtypeStruct((r, d), BF16),
        scratch_shapes=[
            pltpu.VMEM((2, 3, s, dh), BF16),
            pltpu.VMEM((dh, s), BF16), pltpu.VMEM((s, 2 * dh), BF16), pltpu.VMEM((2, qb, s), BF16),
            pltpu.VMEM((s, dh), BF16), pltpu.VMEM((3, r, hw), BF16), pltpu.VMEM((r, 4 * hw), BF16),
            pltpu.VMEM((nk, r, ck), BF16), pltpu.VMEM((ring, ck, nt), BF16), pltpu.VMEM((nn, r, nt), F32),
            pltpu.VMEM((2, r, 2 * nt), BF16), pltpu.VMEM((2, r, 2 * nt), BF16),
            pltpu.SemaphoreType.DMA((2, 3)), pltpu.SemaphoreType.DMA((nk,)), pltpu.SemaphoreType.DMA((ring,)),
            pltpu.SemaphoreType.DMA((2,)), pltpu.SemaphoreType.DMA((2,)),
            pltpu.SemaphoreType.DMA((3,)), pltpu.SemaphoreType.DMA((3,))],
        compiler_params=pltpu.CompilerParams(
            vmem_limit_bytes=63 * 1024 * 1024, collective_id=1,
            has_side_effects=True),
        name="back",
        cost_estimate=_cost(4 * s * s * dh * nh + 2 * r * d * (f + 4 * hw), 2 * d * (f + 4 * hw)),
    )(x, qkv, h, w2, wo)


def _pass_on(y):
    r, d = y.shape
    n = 8
    w = r // n

    def body(y_ref, o_ref, buf, isem, osem):
        def get(i):
            rs = pl.ds(i * w, w)
            return pltpu.make_async_copy(y_ref.at[rs], buf.at[i], isem.at[i])

        def put(i):
            rs = pl.ds(i * w, w)
            return pltpu.make_async_copy(buf.at[i], o_ref.at[rs], osem.at[i])

        for i in range(n):
            get(i).start()
        for i in range(n):
            get(i).wait()
            put(i).start()
        for i in range(n):
            put(i).wait()

    anyspace = pl.BlockSpec(memory_space=pl.ANY)
    return pl.pallas_call(
        body, in_specs=[anyspace], out_specs=anyspace,
        out_shape=jax.ShapeDtypeStruct((r, d), y.dtype),
        scratch_shapes=[pltpu.VMEM((n, w, d), y.dtype), pltpu.SemaphoreType.DMA((n,)),
                        pltpu.SemaphoreType.DMA((n,))],
        compiler_params=pltpu.CompilerParams(vmem_limit_bytes=VMEM), name="pass_on",
        cost_estimate=_cost(0, 4 * r * d),
    )(y)


def solution(mesh):
    nseq = mesh.shape["seq"]

    def local(x, g1, b1, g2, b2, wqkv, wo, w1, w2):
        nh, dh, d = wo.shape
        r = x.shape[0]
        h, qkv = _front(x, g1, b1, g2, b2, jnp.asarray(_inverse_frequencies(dh)), wqkv, w1)
        return _pass_on(_back(x, qkv, h, w2, wo.reshape(nh * dh, d), dh))

    rows = P(("data", "seq"), None)
    rep = P()
    return jax.shard_map(local, mesh=mesh,
                         in_specs=(rows, rep, rep, rep, rep, rep, rep, rep, rep),
                         out_specs=rows, check_vma=False)
```

```python
import functools

import jax
import jax.numpy as jnp
import numpy as np
from jax import lax
from jax.experimental import pallas as pl
from jax.experimental.pallas import tpu as pltpu
from jax.sharding import PartitionSpec as P

EPS = 1e-5
NEG = -1e30
F32 = jnp.float32
BF16 = jnp.bfloat16
VMEM = 60 * 1024 * 1024


def _cost(flops, nbytes):
    return pl.CostEstimate(flops=int(flops), bytes_accessed=int(nbytes), transcendentals=0)


def _dot(a, b):
    return jnp.dot(a, b, preferred_element_type=F32)


MESH = pl.DeviceIdType.MESH
LO = 64


def _inverse_frequencies(dh):
    e = np.arange(dh) % (dh // 2)
    return np.asarray(10000.0 ** (-2.0 * e / dh), np.float32)[None]


def _front(x, g1, b1, g2, b2, inv, wqkv, w1):
    r, d = x.shape
    f = w1.shape[1]
    w3 = wqkv.shape[1] // 3
    hw = w3 // 4
    dh = inv.shape[1]
    highs = 4 * r // LO
    nt = 512
    mt = 2 * nt
    cw = 256
    t1 = f // mt
    nb = hw // nt
    t2 = 3 * nb
    ntile1 = f // nt
    ring = 5
    xc = 128

    def body(x_ref, g1_ref, b1_ref, g2_ref, b2_ref, inv_ref, wqkv_ref, w1_ref,
             h_ref, qkv_ref, x_scr, rows, m_scr, w_scr, t_scr, cos_s, sin_s, h_buf, q_buf,
             xsem, wsem, hsem, qsem, send, recv):
        me = lax.axis_index("seq")
        core = me % 2
        near = me + 1 - 2 * core
        far = (me + 2) % 4

        def member(k):
            return [me, near, far, 3 - me][k]

        def load1(i):
            c = pl.multiple_of(i * nt, nt)
            pltpu.make_async_copy(w1_ref.at[:, pl.ds(c, nt)], w_scr.at[i % ring], wsem.at[i % ring]).start()

        def load2(i):
            slot = (i + ntile1) % ring
            v = i % t2
            c = pl.multiple_of((v // nb) * w3 + me * hw + (v % nb) * nt, nt)
            pltpu.make_async_copy(wqkv_ref.at[:, pl.ds(c, nt)], w_scr.at[slot], wsem.at[slot]).start()

        def ready(i):
            slot = i % ring
            pltpu.make_async_copy(w1_ref.at[:, pl.ds(0, nt)], w_scr.at[slot], wsem.at[slot]).wait()
            return slot

        def remote(src, dst, part, sem, dev):
            return pltpu.make_async_remote_copy(
                src_ref=rows.at[src, part], dst_ref=rows.at[dst, part], send_sem=send.at[sem],
                recv_sem=recv.at[sem], device_id={"seq": dev}, device_id_type=MESH)

        def to_near():
            return remote(0, 1, pl.ds(0, r), 0, near)

        def to_far(p):
            return remote(0, 2, pl.ds(p * (r // 2), r // 2), 1 + p, far)

        def onward(p):
            return remote(2, 3, pl.ds(p * (r // 2), r // 2), 3 + p, near)

        def norm(c, q, _):
            base = c * xc + q * 32
            groups = [pl.ds(pl.multiple_of(base + 16 * g, 16), 16) for g in range(2)]
            nl = d // 128

            def col(rs, j):
                return x_scr[rs, j * 128:(j + 1) * 128].astype(F32)

            def total(f):
                part = [[None] * 4 for _ in groups]
                for j in range(nl):
                    for g, rs in enumerate(groups):
                        v = f(g, col(rs, j))
                        part[g][j % 4] = v if part[g][j % 4] is None else part[g][j % 4] + v
                return [jnp.sum((p[0] + p[1]) + (p[2] + p[3]), axis=-1, keepdims=True) / d for p in part]

            mu = total(lambda g, v: v)
            var = total(lambda g, v: (v - mu[g]) * (v - mu[g]))
            rs_ = [lax.rsqrt(v + EPS) for v in var]
            for j in range(nl):
                cs = slice(j * 128, (j + 1) * 128)
                for g, rs in enumerate(groups):
                    xn = (col(rs, j) - mu[g]) * rs_[g]
                    rows[0, rs, cs] = (xn * g1_ref[:, cs] + b1_ref[:, cs]).astype(BF16)
                    m_scr[rs, cs] = (xn * g2_ref[:, cs] + b2_ref[:, cs]).astype(BF16)
            return 0

        def chunk(c):
            rs = pl.ds(c * xc, xc)
            return pltpu.make_async_copy(x_ref.at[rs], x_scr.at[rs], xsem.at[c])

        for c in range(r // xc):
            chunk(c).start()
        for i in range(ring):
            load1(i)
        bar = pltpu.get_barrier_semaphore()
        for dev in (near, far):
            pl.semaphore_signal(bar, inc=1, device_id={"seq": dev}, device_id_type=MESH)
        neg = lax.broadcasted_iota(jnp.int32, (LO, dh), 1) < dh // 2
        lo = lax.broadcasted_iota(jnp.int32, (LO, dh), 0).astype(F32) * inv_ref[...]
        hi = (LO * lax.broadcasted_iota(jnp.int32, (highs, dh), 0)).astype(F32) * inv_ref[...]
        cl, sl = jnp.cos(lo), jnp.sin(lo)
        cos_s[0, :highs, :] = jnp.cos(hi)
        sin_s[0, :highs, :] = jnp.sin(hi)
        n = r // LO
        tables = []
        for k in range(4):
            base = pl.ds(pl.multiple_of(member(k) * n, n), n)
            tables.append((cos_s[0, base, :], sin_s[0, base, :]))
        for k, (hc, hs) in enumerate(tables):
            for i in range(n):
                a, b = hc[i:i + 1], hs[i:i + 1]
                sn = b * cl + a * sl
                cos_s[k, i * LO:(i + 1) * LO, :] = a * cl - b * sl
                sin_s[k, i * LO:(i + 1) * LO, :] = jnp.where(neg, -sn, sn)
        for c in range(r // xc):
            chunk(c).wait()
            lax.fori_loop(0, xc // 32, functools.partial(norm, c), 0)
            if c == r // xc // 2 - 1:
                pl.semaphore_wait(bar, 2)
                to_far(0).start()
        to_far(1).start()
        to_near().start()

        def h_out(i):
            c = pl.multiple_of(i * mt, mt)
            return pltpu.make_async_copy(h_buf.at[i % 2], h_ref.at[:, pl.ds(c, mt)], hsem.at[i % 2])

        def q_out(i):
            v = i % t2
            chip = me // 2
            pair = chip + (i // t2) * (1 - 2 * chip)
            rs = pl.ds(pl.multiple_of(pair * 2 * r, 2 * r), 2 * r)
            c = pl.multiple_of(v * nt, nt)
            return pltpu.make_async_copy(q_buf.at[i % 2], qkv_ref.at[rs, pl.ds(c, nt)], qsem.at[i % 2])


        def gelu(i, cols):
            t = t_scr[:, cols]
            h_buf[i % 2, :, cols] = (0.5 * t * (1.0 + lax.erf(t * (0.5 ** 0.5)))).astype(BF16)

        def mlp(s, first):
            slots = [ready(2 * s + half) for half in range(mt // nt)]
            for half, slot in enumerate(slots):
                for c in range(nt // cw):
                    cols = slice(half * nt + c * cw, half * nt + (c + 1) * cw)
                    if not first:
                        gelu(s - 1, cols)
                    t_scr[:, cols] = _dot(m_scr[...], w_scr[slot, :, c * cw:(c + 1) * cw])
            if not first:
                h_out(s - 1).start()

        def rope(i, j):
            isv = (i % t2) // nb == 2
            base = 2 * (i // t2)
            k, c = j // (nt // cw), j % (nt // cw)
            out = pl.ds(pl.multiple_of((core if k == 0 else 1 - core) * r, r), r)
            t = t_scr[:, j * cw:(j + 1) * cw].astype(BF16).astype(F32)
            for hd in range(cw // dh):
                p = t[:, hd * dh:(hd + 1) * dh]
                v = p * cos_s[base + k] + pltpu.roll(p, dh // 2, 1) * sin_s[base + k]
                lo = c * cw + hd * dh
                q_buf[i % 2, out, lo:lo + dh] = jnp.where(isv, p, v).astype(BF16)

        def qkv(u, first):
            slot = ready(ntile1 + u)
            base = 2 * (u // t2)
            for j in range(mt // cw):
                cols = slice(j * cw, (j + 1) * cw)
                k, c = j // (nt // cw), j % (nt // cw)
                if first:
                    gelu(t1 - 1, cols)
                else:
                    rope(u - 1, j)
                t_scr[:, cols] = _dot(rows[base + k], w_scr[slot, :, c * cw:(c + 1) * cw])

        mlp(0, True)
        load1(ring)
        load1(ring + 1)

        inner = (ntile1 - ring - 2) // 2 + 1

        def mlp_step(s, _):
            @pl.when(s > 2)
            def _():
                h_out(s - 3).wait()

            mlp(s, False)

            @pl.when(s < inner)
            def _():
                load1(2 * s + ring)
                load1(2 * s + ring + 1)

            @pl.when(s >= inner)
            def _():
                i = 2 * s + ring

                @pl.when(i < ntile1)
                def _():
                    load1(i)

                @pl.when(i >= ntile1)
                def _():
                    load2(i - ntile1)

                load2(i + 1 - ntile1)
            return 0

        lax.fori_loop(1, t1, mlp_step, 0)

        to_near().wait_recv()
        to_far(0).wait_recv()
        onward(0).start()
        h_out(t1 - 3).wait()
        qkv(0, True)
        h_out(t1 - 1).start()
        load2(ring)

        def qkv_step(u, _):
            @pl.when(u == t2 - 2)
            def _():
                to_far(1).wait_recv()
                onward(1).start()

            @pl.when(u == t2)
            def _():
                onward(0).wait_recv()
                onward(1).wait_recv()

            @pl.when(u > 2)
            def _():
                q_out(u - 3).wait()

            qkv(u, False)
            q_out(u - 1).start()

            @pl.when(u + ring < 2 * t2)
            def _():
                load2(u + ring)
            return 0

        lax.fori_loop(1, 2 * t2, qkv_step, 0)
        q_out(2 * t2 - 3).wait()
        for j in range(mt // cw):
            rope(2 * t2 - 1, j)
        q_out(2 * t2 - 1).start()
        h_out(t1 - 2).wait()
        h_out(t1 - 1).wait()
        q_out(2 * t2 - 2).wait()
        q_out(2 * t2 - 1).wait()
        to_near().wait_send()
        for p in range(2):
            to_far(p).wait_send()
            onward(p).wait_send()

    anyspace = pl.BlockSpec(memory_space=pl.ANY)
    inside = pl.BlockSpec(memory_space=pltpu.VMEM)
    return pl.pallas_call(
        body,
        in_specs=[anyspace] + [inside] * 5 + [anyspace] * 2,
        out_specs=[anyspace, anyspace],
        out_shape=[jax.ShapeDtypeStruct((r, f), BF16), jax.ShapeDtypeStruct((4 * r, 3 * hw), BF16)],
        scratch_shapes=[
            pltpu.VMEM((r, d), BF16), pltpu.VMEM((4, r, d), BF16), pltpu.VMEM((r, d), BF16),
            pltpu.VMEM((ring, d, nt), BF16),
            pltpu.VMEM((r, mt), F32), pltpu.VMEM((4, r, dh), F32), pltpu.VMEM((4, r, dh), F32),
            pltpu.VMEM((2, r, mt), BF16), pltpu.VMEM((2, 2 * r, nt), BF16),
            pltpu.SemaphoreType.DMA((r // xc,)), pltpu.SemaphoreType.DMA((ring,)),
            pltpu.SemaphoreType.DMA((2,)), pltpu.SemaphoreType.DMA((2,)),
            pltpu.SemaphoreType.DMA((5,)), pltpu.SemaphoreType.DMA((5,))],
        compiler_params=pltpu.CompilerParams(
            vmem_limit_bytes=VMEM, collective_id=0, has_side_effects=True),
        name="front",
        cost_estimate=_cost(2 * r * d * f + 2 * 4 * r * d * 3 * hw, 2 * d * f + 4 * d * 3 * hw),
    )(x, g1[None], b1[None], g2[None], b2[None], inv, wqkv, w1)


def _back(x, qkv, h, w2, wo, dh):
    r, d = x.shape
    s, w = qkv.shape
    f = h.shape[1]
    hw = w // 3
    nh = hw // dh
    qb = 256
    c2 = dh ** -0.5 * 1.4426950408889634
    nblk = s // qb
    nt = 512
    cw = 256
    ck = 4096
    nk = f // ck
    nn = d // nt
    ring = 4
    to = nn // 2
    ntile2 = nn * nk

    def body(x_ref, qkv_ref, h_ref, w2_ref, wo_ref, y_ref,
             qkv_buf, kt, vx, pb, o_scr, o_send, o_all, h_scr, w_scr, acc, x_buf, y_buf,
             asem, hsem, wsem, xsem, ysem, send, recv):
        me = lax.axis_index("seq")
        near = me + 1 - 2 * (me % 2)
        members = [me, near, (me + 2) % 4, 3 - me]

        def load(i, wo=False):
            slot = i % ring
            if wo:
                src = wo_ref.at[:, pl.ds(pl.multiple_of((i - ntile2) * nt, nt), nt)]
            else:
                rows = pl.ds(pl.multiple_of((i % nk) * ck, ck), ck)
                src = w2_ref.at[rows, pl.ds(pl.multiple_of((i // nk) * nt, nt), nt)]
            pltpu.make_async_copy(src, w_scr.at[slot], wsem.at[slot]).start()

        def heads(i):
            return [pltpu.make_async_copy(
                qkv_ref.at[:, pl.ds(pl.multiple_of(t * hw + i * dh, dh), dh)],
                qkv_buf.at[i % 2, t], asem.at[i % 2, t]) for t in range(3)]

        def x_in(i):
            cols = pl.ds(pl.multiple_of(i * 2 * nt, 2 * nt), 2 * nt)
            return pltpu.make_async_copy(x_ref.at[:, cols], x_buf.at[i % 2], xsem.at[i % 2])

        def y_out(i):
            cols = pl.ds(pl.multiple_of(i * 2 * nt, 2 * nt), 2 * nt)
            return pltpu.make_async_copy(y_buf.at[i % 2], y_ref.at[:, cols], ysem.at[i % 2])

        def ready(i):
            slot = i % ring
            pltpu.make_async_copy(wo_ref.at[:, pl.ds(0, nt)], w_scr.at[slot], wsem.at[slot]).wait()
            return slot

        def hcopy(c):
            return pltpu.make_async_copy(h_ref.at[:, pl.ds(c * ck, ck)], h_scr.at[c], hsem.at[c])

        def share(k):
            return pltpu.make_async_remote_copy(
                src_ref=o_send.at[k - 1],
                dst_ref=o_all.at[:, pl.ds(pl.multiple_of(me * hw, hw), hw)],
                send_sem=send.at[k - 1], recv_sem=recv.at[k - 1],
                device_id={"seq": members[k]}, device_id_type=MESH)

        for t in heads(0):
            t.start()
        bar = pltpu.get_barrier_semaphore()
        for k in range(1, 4):
            pl.semaphore_signal(bar, inc=1, device_id={"seq": members[k]}, device_id_type=MESH)
        vx[:, dh:] = jnp.ones((s, dh), BF16)

        row = lax.broadcasted_iota(jnp.int32, (qb, qb), 0)
        col = lax.broadcasted_iota(jnp.int32, (qb, qb), 1)
        keep = col <= row

        def scores(i, b, w):
            q = qkv_buf[i % 2, 0, b * qb:(b + 1) * qb, :]
            m = None
            for c in range(b + 1):
                cols = slice(c * qb, (c + 1) * qb)
                t = _dot(q, kt[:, cols])
                if c == b:
                    t = jnp.where(keep, t, NEG)
                acc[w * (s // nt) + c * qb // nt, :qb, (c * qb) % nt:(c * qb) % nt + qb] = t
                for g in range(qb // dh):
                    u = t[:, g * dh:(g + 1) * dh]
                    m = u if m is None else jnp.maximum(m, u)
            return jnp.max(m, axis=-1, keepdims=True) * c2

        def finish(b, m, w):
            n = (b + 1) * qb
            for c in range(b + 1):
                t = acc[w * (s // nt) + c * qb // nt, :qb, (c * qb) % nt:(c * qb) % nt + qb]
                pb[w, :, c * qb:(c + 1) * qb] = jnp.exp2(t * c2 - m).astype(BF16)
            o = _dot(pb[w, :, :n], vx[:n, :])
            o_scr[b * qb:n, :] = (o[:, :dh] / o[:, dh:]).astype(BF16)

        def head(i, _):
            @pl.when(i + 1 < nh)
            def _():
                for t in heads(i + 1):
                    t.start()

            for c in range(nk):
                @pl.when(i == c)
                def _(c=c):
                    hcopy(c).start()

            for c in range(ring):
                @pl.when(i == nh - ring + c)
                def _(c=c):
                    load(c)

            for t in heads(i):
                t.wait()
            for c in range(nblk):
                cols = slice(c * qb, (c + 1) * qb)
                vx[cols, :dh] = qkv_buf[i % 2, 2, cols, :]
                kt[:, cols] = qkv_buf[i % 2, 1, cols, :].T
            order = [nblk // 2 - 1] + [b for b in range(nblk)[::-1] if b != nblk // 2 - 1]
            m = scores(i, order[0], 0)
            for j, b in enumerate(order):
                ahead = scores(i, order[j + 1], (j + 1) % 2) if j + 1 < nblk else None
                finish(b, m, j % 2)
                m = ahead
            own = pl.ds(pl.multiple_of(me * r, r), r)
            lanes = pl.ds(pl.multiple_of(i * dh, dh), dh)
            o_all[:, pl.ds(pl.multiple_of(me * hw + i * dh, dh), dh)] = o_scr[own, :]
            for k in range(1, 4):
                o_send[k - 1, :, lanes] = o_scr[pl.ds(pl.multiple_of(members[k] * r, r), r), :]
            return 0

        lax.fori_loop(0, nh, head, 0)
        pl.semaphore_wait(bar, 3)
        for k in (2, 3, 1):
            share(k).start()
        for c in range(nk):
            hcopy(c).wait()

        def second(n, half):
            slots = [ready(nk * n + 2 * half), ready(nk * n + 2 * half + 1)]
            kc = 2 * half
            for c in range(nt // cw):
                cols = slice(c * cw, (c + 1) * cw)
                t = _dot(h_scr[kc], w_scr[slots[0], :, cols]) + _dot(h_scr[kc + 1], w_scr[slots[1], :, cols])
                acc[n, :, cols] = acc[n, :, cols] + t if half else t

        def w2_step(n, _):
            for half in range(nk // 2):
                second(n, half)

                @pl.when(n < nn - 1)
                def _():
                    load(nk * (n + 1) + 2 * half)
                    load(nk * (n + 1) + 2 * half + 1)

                @pl.when(n == nn - 1)
                def _():
                    load(nk * nn + 2 * half, wo=True)
                    load(nk * nn + 2 * half + 1, wo=True)
            return 0

        x_in(0).start()
        lax.fori_loop(0, nn, w2_step, 0)
        for k in range(1, 4):
            share(k).wait_recv()

        def wo_step(n, _):
            @pl.when(n + 1 < to)
            def _():
                x_in(n + 1).start()

            x_in(n).wait()

            @pl.when(n > 1)
            def _():
                y_out(n - 2).wait()

            slots = [ready(ntile2 + 2 * n), ready(ntile2 + 2 * n + 1)]
            for half, slot in enumerate(slots):
                for c in range(nt // cw):
                    cols = slice(c * cw, (c + 1) * cw)
                    out = slice(half * nt + c * cw, half * nt + (c + 1) * cw)
                    t = _dot(o_all[...], w_scr[slot, :, cols])
                    t = (x_buf[n % 2, :, out].astype(F32) + t) + acc[2 * n + half, :, cols]
                    y_buf[n % 2, :, out] = t.astype(BF16)
            y_out(n).start()

            @pl.when(n + 2 < to)
            def _():
                load(ntile2 + 2 * n + ring, wo=True)
                load(ntile2 + 2 * n + ring + 1, wo=True)
            return 0

        lax.fori_loop(0, to, wo_step, 0)
        y_out(to - 2).wait()
        y_out(to - 1).wait()
        for k in range(1, 4):
            share(k).wait_send()

    anyspace = pl.BlockSpec(memory_space=pl.ANY)
    return pl.pallas_call(
        body,
        in_specs=[anyspace] * 5,
        out_specs=anyspace,
        out_shape=jax.ShapeDtypeStruct((r, d), BF16),
        scratch_shapes=[
            pltpu.VMEM((2, 3, s, dh), BF16),
            pltpu.VMEM((dh, s), BF16), pltpu.VMEM((s, 2 * dh), BF16), pltpu.VMEM((2, qb, s), BF16),
            pltpu.VMEM((s, dh), BF16), pltpu.VMEM((3, r, hw), BF16), pltpu.VMEM((r, 4 * hw), BF16),
            pltpu.VMEM((nk, r, ck), BF16), pltpu.VMEM((ring, ck, nt), BF16), pltpu.VMEM((nn, r, nt), F32),
            pltpu.VMEM((2, r, 2 * nt), BF16), pltpu.VMEM((2, r, 2 * nt), BF16),
            pltpu.SemaphoreType.DMA((2, 3)), pltpu.SemaphoreType.DMA((nk,)), pltpu.SemaphoreType.DMA((ring,)),
            pltpu.SemaphoreType.DMA((2,)), pltpu.SemaphoreType.DMA((2,)),
            pltpu.SemaphoreType.DMA((3,)), pltpu.SemaphoreType.DMA((3,))],
        compiler_params=pltpu.CompilerParams(
            vmem_limit_bytes=63 * 1024 * 1024, collective_id=1,
            has_side_effects=True),
        name="back",
        cost_estimate=_cost(4 * s * s * dh * nh + 2 * r * d * (f + 4 * hw), 2 * d * (f + 4 * hw)),
    )(x, qkv, h, w2, wo)


def _pass_on(y):
    r, d = y.shape
    n = 8
    w = r // n

    def body(y_ref, o_ref, buf, isem, osem):
        def get(i):
            rs = pl.ds(i * w, w)
            return pltpu.make_async_copy(y_ref.at[rs], buf.at[i], isem.at[i])

        def put(i):
            rs = pl.ds(i * w, w)
            return pltpu.make_async_copy(buf.at[i], o_ref.at[rs], osem.at[i])

        for i in range(n):
            get(i).start()
        for i in range(n):
            get(i).wait()
            put(i).start()
        for i in range(n):
            put(i).wait()

    anyspace = pl.BlockSpec(memory_space=pl.ANY)
    return pl.pallas_call(
        body, in_specs=[anyspace], out_specs=anyspace,
        out_shape=jax.ShapeDtypeStruct((r, d), y.dtype),
        scratch_shapes=[pltpu.VMEM((n, w, d), y.dtype), pltpu.SemaphoreType.DMA((n,)),
                        pltpu.SemaphoreType.DMA((n,))],
        compiler_params=pltpu.CompilerParams(vmem_limit_bytes=VMEM), name="pass_on",
        cost_estimate=_cost(0, 4 * r * d),
    )(y)


def solution(mesh):
    nseq = mesh.shape["seq"]

    def local(x, g1, b1, g2, b2, wqkv, wo, w1, w2):
        nh, dh, d = wo.shape
        r = x.shape[0]
        h, qkv = _front(x, g1, b1, g2, b2, jnp.asarray(_inverse_frequencies(dh)), wqkv, w1)
        return _pass_on(_back(x, qkv, h, w2, wo.reshape(nh * dh, d), dh))

    rows = P(("data", "seq"), None)
    rep = P()
    return jax.shard_map(local, mesh=mesh,
                         in_specs=(rows, rep, rep, rep, rep, rep, rep, rep, rep),
                         out_specs=rows, check_vma=False)
```
